512 devices in a mesh: sensor: 128 (over y_lo, z, x, core), batch: 4 (over y_hi).
Axes of the slice: x: 4, y: 8 (y_hi: 4, y_lo: 2; y = y_hi * 2 + y_lo), z: 8, core: 2. Of those that a mesh axis runs over, the one named last changes fastest.
Arguments:
- samples: bfloat16 [512, 262144], P('batch', 'sensor'), may hold values from -24 to 24
- branch_weight: bfloat16 [262144, 2048], P('sensor', 'batch'), may hold values from -0.01171875 to 0.01171875
- branch_bias: float32 [2048], P('batch'), may hold values from -3 to 3
- upstream: bfloat16 [512, 2048], P('sensor', 'batch'), may hold values from -0.29882812 to 0.29882812
Outputs:
- activation: bfloat16 [512, 2048], P('sensor', 'batch')
- weight_grad: bfloat16 [262144, 2048], P('sensor', 'batch')
- bias_grad: float32 [2048], P('batch')
The draws below stay inside these ranges and needn't reach their ends.
All inputs are finite; a program needn't handle non-finite values.
Results may differ from the reference program's by a relative error of at most 0.005.
Values may be sent and summed in bfloat16 or wider, within the bound.
A program may use at most 64 MiB of HBM per device.

```python
import jax
import jax.numpy as jnp
from jax import lax

HIDDEN_SIZE = 2048
SENSORS = 262144
FUNCS = 512


def spiked(result, stream_key, source, target, parts, factor):
    owner, partner = [(jnp.arange(result.shape[axis_at]) // (result.shape[axis_at] // parts)).reshape([-1 if axis == axis_at else 1 for axis in range(result.ndim)]) for axis_at in (source, target)]
    chosen = jax.random.permutation(stream_key, parts)[partner]
    strong = (owner == chosen) | (owner == (partner + parts // 2) % parts)
    return jnp.where(strong, factor * result, result)


def block_scale(own_key, shape, split, low, top_value):
    gain = 1.0
    for axis_at, parts in split:
        steps = jax.random.uniform(jax.random.fold_in(jax.random.fold_in(own_key, 6), axis_at), (parts,), jnp.float32, low / len(split), top_value / len(split))
        gain = gain * jnp.repeat(jnp.exp(steps), shape[axis_at] // parts).reshape((-1,) + (1,) * (len(shape) - 1 - axis_at))
    return gain


def centred(own_key, shape, deviation, limit, split=(), kind=jnp.bfloat16):
    result = deviation * jax.random.normal(own_key, shape, jnp.float32)
    if split:
        result = result * block_scale(own_key, shape, split, -0.22, 0.18)
    return jnp.clip(result, -limit, limit).astype(kind)


def heavy_noise(stream_key, shape, spread, limit, pieces, heavy, held_as=jnp.bfloat16):
    result = spread * jax.random.normal(stream_key, shape, jnp.float32)
    if pieces:
        result = result * block_scale(stream_key, shape, pieces, -0.22, 0.18)
    return jnp.clip(spiked(result, jax.random.fold_in(stream_key, 3), *heavy), -limit, limit).astype(held_as)


def setup_inputs(seed: int = 0) -> dict:
    seeds = jax.random.split(jax.random.key(seed), 5)
    samples = heavy_noise(seeds[0], (FUNCS, SENSORS), 1.0, 24.0, ((0, 4), (1, 128)), (1, 0, 128, 5.5))
    branch_weight = centred(seeds[1], (SENSORS, HIDDEN_SIZE), SENSORS ** -0.5, 0.01171875, ((0, 128), (1, 4)))
    branch_bias = centred(seeds[2], (HIDDEN_SIZE,), 0.5, 3.0, ((0, 4),), jnp.float32)
    upstream = centred(seeds[3], (FUNCS, HIDDEN_SIZE), 0.05, 0.29882812, ((0, 128), (1, 4)))
    return dict(samples=samples, branch_weight=branch_weight, branch_bias=branch_bias, upstream=upstream)


def reference(samples, branch_weight, branch_bias, upstream):
    pre = jnp.dot(samples, branch_weight, preferred_element_type=jnp.float32) + branch_bias.astype(jnp.float32)[None, :]
    act_full = jnp.tanh(pre)
    activation = act_full.astype(jnp.bfloat16)
    grad_pre = (upstream.astype(jnp.float32) * (1.0 - act_full * act_full)).astype(jnp.bfloat16)
    weight_grad = lax.dot_general(samples, grad_pre, (((0,), (0,)), ((), ())), preferred_element_type=jnp.float32).astype(jnp.bfloat16)
    bias_grad = jnp.sum(grad_pre.astype(jnp.float32), axis=0)
    return activation, weight_grad, bias_grad
```

```python
import jax
import jax.numpy as jnp
from jax import lax
from jax.experimental import pallas as pl
from jax.experimental.pallas import tpu as pltpu
from jax.sharding import Mesh
from jax.sharding import PartitionSpec as P

SENSOR = ("y_lo", "z", "x", "core")
STEPS = 8
ROWS = 32
OWNED = 4
CLASSES = 8
DEPTH = 8
TILE = 256


def group_of(batch, step, half):
    own = step // 2 == 0
    far = step // 2 == 3
    block = jnp.where(own, batch, jnp.where(far, batch + 2, batch + 3 + 2 * half))
    piece = jnp.where(own, 2 * step + half, jnp.where(far, step - 6 + 2 * half, step - 2))
    return lax.rem(block, 4) * 4 + piece


def slot_of(batch, group):
    away = lax.rem(group // 4 + 4 - batch, 4)
    piece = lax.rem(group, 4)
    near = 4 + 2 * piece + jnp.where(away == 1, 1, 0)
    far = 12 + 2 * lax.rem(piece, 2) + piece // 2
    return jnp.where(away == 0, piece, jnp.where(away == 2, far, near))


def kernel(
    samples, weight, bias, upstream,
    act_out, grad_out, bias_out,
    s_buf, w_buf, st_buf, out_buf,
    a_send_buf, a_buf, b_send_buf, b_buf, z_buf, c_buf,
    part, asm, g_buf, u_buf, u_pair, act_buf,
    load_sem, w_sem, u_sem, y_send, y_recv, us_sem, ur_sem, uz_send, uz_recv,
    a_send, a_recv, b_send, b_recv, z_send, z_recv, c_send, c_recv, out_sem,
):
    y_lo, z, x, core = (lax.axis_index(name) for name in SENSOR)
    batch = lax.axis_index("batch")
    mine = 2 * x + core
    up, down = lax.rem(batch + 1, 4), lax.rem(batch + 3, 4)
    other = 1 - y_lo

    def class_peer(d):
        k = lax.rem(mine + d, CLASSES)
        return k, {"x": k // 2, "core": lax.rem(k, 2)}

    def z_peer(d):
        return {"z": lax.rem(z + d, DEPTH)}

    loads = [
        pltpu.make_async_copy(samples.at[pl.ds(ROWS * j, ROWS)], s_buf.at[j], load_sem.at[j]) for j in range(4)
    ]
    for copy in loads:
        copy.start()
    load_w = pltpu.make_async_copy(weight, w_buf, w_sem)
    load_w.start()
    load_u = pltpu.make_async_copy(upstream, u_buf.at[z, y_lo], u_sem)
    load_u.start()

    barrier = pltpu.get_barrier_semaphore()
    for peer in (up, down):
        pl.semaphore_signal(barrier, inc=1, device_id={"batch": peer})
    pl.semaphore_signal(barrier, inc=1, device_id={"y_lo": other})
    for d in range(1, CLASSES):
        pl.semaphore_signal(barrier, inc=1, device_id=class_peer(d)[1])
    for d in range(1, DEPTH):
        pl.semaphore_signal(barrier, inc=1, device_id=z_peer(d))
    for copy in loads:
        copy.wait()
    pl.semaphore_wait(barrier, 3 + CLASSES - 1 + DEPTH - 1)

    def y_copy(source, target, direction, index):
        return pltpu.make_async_remote_copy(
            src_ref=s_buf.at[source],
            dst_ref=s_buf.at[target],
            send_sem=y_send.at[direction, index],
            recv_sem=y_recv.at[target],
            device_id={"batch": up if direction == 0 else down},
        )

    sends = []
    for j in range(4):
        for direction in range(2):
            copy = y_copy(j, 4 + 2 * j + direction, direction, j)
            copy.start()
            sends.append(copy)
    forwards = {}
    for j in range(2):
        forwards[2 + j] = y_copy(4 + 2 * j, 12 + 2 * j, 0, 4 + j)
        forwards[4 + j] = y_copy(4 + 2 * (2 + j) + 1, 12 + 2 * j + 1, 1, 4 + j)

    load_u.wait()
    u_cross = pltpu.make_async_remote_copy(
        src_ref=u_buf.at[z, y_lo], dst_ref=u_buf.at[z, y_lo], send_sem=us_sem, recv_sem=ur_sem,
        device_id={"y_lo": other},
    )
    u_cross.start()
    load_w.wait()

    def spread(source, target, send_sem, recv_sem, peers):
        for device in peers:
            pltpu.make_async_remote_copy(
                src_ref=source, dst_ref=target, send_sem=send_sem, recv_sem=recv_sem, device_id=device
            ).start()

    def await_bytes(region, sem):
        pltpu.make_async_copy(region, region, sem).wait()

    def stage_matmul(p):
        rows = s_buf[pl.ds(2 * p, 2)].reshape(2 * ROWS, s_buf.shape[-1])
        part[...] = jnp.dot(rows, w_buf[...], preferred_element_type=jnp.float32)
        for half in range(2):
            for k in range(CLASSES):
                a_send_buf[p, k, OWNED * half : OWNED * (half + 1), :] = part[
                    ROWS * half + OWNED * k : ROWS * half + OWNED * (k + 1), :
                ]
        for d in range(1, CLASSES):
            k, device = class_peer(d)
            spread(a_send_buf.at[p, k], a_buf.at[p, mine], a_send.at[p], a_recv.at[p], [device])

    def stage_class_sum(p):
        await_bytes(a_buf.at[p, pl.ds(0, CLASSES - 1)], a_recv.at[p])
        total = a_send_buf[p, mine]
        for d in range(1, CLASSES):
            total = total + a_buf[p, lax.rem(mine + d, CLASSES)]
        b_send_buf[p] = total
        spread(b_send_buf.at[p], b_buf.at[p], b_send.at[p], b_recv.at[p], [{"y_lo": other}])

    def stage_pair_sum(p):
        await_bytes(b_buf.at[p], b_recv.at[p])
        z_buf[p, z] = b_send_buf[p] + b_buf[p]
        spread(z_buf.at[p, z], z_buf.at[p, z], z_send.at[p], z_recv.at[p], [z_peer(d) for d in range(1, DEPTH)])

    def stage_gradient(p):
        await_bytes(z_buf.at[p, pl.ds(0, DEPTH - 1)], z_recv.at[p])
        total = z_buf[p, 0]
        for i in range(1, DEPTH):
            total = total + z_buf[p, i]
        act = jnp.tanh(total + bias[...])
        for half in range(2):
            group = group_of(batch, p, half)
            rows = slice(OWNED * half, OWNED * (half + 1))
            u_pair[rows, :] = u_buf[lax.rem(group, DEPTH), group // DEPTH].astype(jnp.float32)
            act_buf[2 * p + half] = act[rows]
        grad = (u_pair[...] * (1.0 - act * act)).astype(jnp.bfloat16).astype(jnp.float32)
        c_buf[p, mine] = grad
        spread(
            c_buf.at[p, mine], c_buf.at[p, mine], c_send.at[p], c_recv.at[p],
            [class_peer(d)[1] for d in range(1, CLASSES)],
        )

    def stage_assemble(p):
        await_bytes(c_buf.at[p, pl.ds(0, CLASSES - 1)], c_recv.at[p])
        for half in range(2):
            for k in range(CLASSES):
                asm[ROWS * half + OWNED * k : ROWS * half + OWNED * (k + 1), :] = c_buf[
                    p, k, OWNED * half : OWNED * (half + 1), :
                ]
        grads = asm[...]
        g_buf[pl.ds(pl.multiple_of(2 * ROWS * p, 2 * ROWS), 2 * ROWS)] = grads.astype(jnp.bfloat16)
        bias_out[...] += jnp.sum(grads, axis=0, keepdims=True)

    def turn(block):
        rows = s_buf[4 * block : 4 * block + 4].reshape(4 * ROWS, s_buf.shape[-1])
        st_buf[:, 4 * ROWS * block : 4 * ROWS * (block + 1)] = rows.T

    bias_out[...] = jnp.zeros_like(bias_out)
    u_cross.wait()
    spread(u_buf.at[z], u_buf.at[z], uz_send, uz_recv, [z_peer(d) for d in range(1, DEPTH)])
    turn(0)

    @pl.loop(0, STEPS + 4)
    def _(s):
        @pl.when(s >= 4)
        def _():
            stage_assemble(s - 4)

        @pl.when(s == 3)
        def _():
            await_bytes(u_buf.at[pl.ds(0, DEPTH - 1)], uz_recv)

        @pl.when((s >= 3) & (s < STEPS + 3))
        def _():
            stage_gradient(s - 3)

        @pl.when((s >= 2) & (s < STEPS + 2))
        def _():
            stage_pair_sum(s - 2)

        @pl.when((s >= 1) & (s < STEPS + 1))
        def _():
            stage_class_sum(s - 1)

        @pl.when(s == 4)
        def _():
            turn(1)

        @pl.when(s == 6)
        def _():
            turn(2)

        for p in range(2, STEPS):
            @pl.when(s == p)
            def _(p=p):
                for half in range(2):
                    y_copy(2 * p + half, 2 * p + half, half, 0).wait_recv()
                if p in forwards:
                    forwards[p].start()

        @pl.when(s < STEPS)
        def _():
            stage_matmul(s)

        @pl.when(s == STEPS - 1)
        def _():
            turn(3)

    act_out[...] = act_buf[slot_of(batch, y_lo * DEPTH + z)].astype(jnp.bfloat16)

    tiles = st_buf.shape[0] // TILE

    def out_copy(t):
        rows = pl.ds(pl.multiple_of(t * TILE, TILE), TILE)
        return pltpu.make_async_copy(out_buf.at[rows], grad_out.at[rows], out_sem.at[t])

    @pl.loop(0, tiles)
    def _(t):
        rows = pl.ds(pl.multiple_of(t * TILE, TILE), TILE)
        out_buf[rows] = jnp.dot(st_buf[rows], g_buf[...], preferred_element_type=jnp.float32).astype(jnp.bfloat16)
        out_copy(t).start()

    for copy in sends:
        copy.wait_send()
    for copy in forwards.values():
        copy.wait_send()
    await_bytes(u_buf.at[pl.ds(0, DEPTH - 1)], uz_send)

    @pl.loop(0, STEPS)
    def _(p):
        await_bytes(a_buf.at[p, pl.ds(0, CLASSES - 1)], a_send.at[p])
        await_bytes(b_buf.at[p], b_send.at[p])
        await_bytes(z_buf.at[p, pl.ds(0, DEPTH - 1)], z_send.at[p])
        await_bytes(c_buf.at[p, pl.ds(0, CLASSES - 1)], c_send.at[p])

    @pl.loop(0, tiles)
    def _(t):
        out_copy(t).wait()


def body(samples, branch_weight, branch_bias, upstream):
    sensors, hidden = branch_weight.shape
    funcs = 4 * samples.shape[0]
    share = 2 * OWNED
    f32, bf16 = jnp.float32, jnp.bfloat16
    dma = pltpu.SemaphoreType.DMA
    tiles = sensors // TILE
    activation, weight_grad, bias_grad = pl.pallas_call(
        kernel,
        out_shape=(
            jax.ShapeDtypeStruct((OWNED, hidden), bf16),
            jax.ShapeDtypeStruct((sensors, hidden), bf16),
            jax.ShapeDtypeStruct((1, hidden), f32),
        ),
        in_specs=[
            pl.BlockSpec(memory_space=pl.ANY),
            pl.BlockSpec(memory_space=pl.ANY),
            pl.BlockSpec(memory_space=pltpu.VMEM),
            pl.BlockSpec(memory_space=pl.ANY),
        ],
        out_specs=(
            pl.BlockSpec(memory_space=pltpu.VMEM),
            pl.BlockSpec(memory_space=pl.ANY),
            pl.BlockSpec(memory_space=pltpu.VMEM),
        ),
        scratch_shapes=[
            pltpu.VMEM((2 * STEPS, ROWS, sensors), bf16),
            pltpu.VMEM((sensors, hidden), bf16),
            pltpu.VMEM((sensors, funcs), bf16),
            pltpu.VMEM((sensors, hidden), bf16),
            pltpu.VMEM((STEPS, CLASSES, share, hidden), f32),
            pltpu.VMEM((STEPS, CLASSES, share, hidden), f32),
            pltpu.VMEM((STEPS, share, hidden), f32),
            pltpu.VMEM((STEPS, share, hidden), f32),
            pltpu.VMEM((STEPS, DEPTH, share, hidden), f32),
            pltpu.VMEM((STEPS, CLASSES, share, hidden), f32),
            pltpu.VMEM((2 * ROWS, hidden), f32),
            pltpu.VMEM((2 * ROWS, hidden), f32),
            pltpu.VMEM((funcs, hidden), bf16),
            pltpu.VMEM((DEPTH, 2, OWNED, hidden), bf16),
            pltpu.VMEM((share, hidden), f32),
            pltpu.VMEM((2 * STEPS, OWNED, hidden), f32),
            dma((4,)), dma, dma, dma((2, 6)), dma((2 * STEPS,)), dma, dma, dma, dma,
            dma((STEPS,)), dma((STEPS,)), dma((STEPS,)), dma((STEPS,)),
            dma((STEPS,)), dma((STEPS,)), dma((STEPS,)), dma((STEPS,)),
            dma((tiles,)),
        ],
        compiler_params=pltpu.CompilerParams(
            collective_id=0, has_side_effects=True, vmem_limit_bytes=48 * 1024 * 1024
        ),
    )(samples, branch_weight, branch_bias[None, :], upstream)
    return activation, weight_grad, bias_grad[0]


def solution(mesh):
    torus = Mesh(
        mesh.devices.reshape(2, 8, 4, 2, mesh.shape["batch"]),
        (*SENSOR, "batch"),
    )
    in_specs = (P("batch", SENSOR), P(SENSOR, "batch"), P("batch"), P(SENSOR, "batch"))
    out_specs = (P(SENSOR, "batch"), P(SENSOR, "batch"), P("batch"))
    return jax.shard_map(body, mesh=torus, in_specs=in_specs, out_specs=out_specs, check_vma=False)
```

```python
import jax
import jax.numpy as jnp
from jax import lax
from jax.experimental import pallas as pl
from jax.experimental.pallas import tpu as pltpu
from jax.sharding import Mesh
from jax.sharding import PartitionSpec as P

SENSOR = ("y_lo", "z", "x", "core")
STEPS = 8
ROWS = 32
PIECE = 16
AHEAD = 3
OWNED = 4
CLASSES = 8
DEPTH = 8
TILE = 256


def group_of(batch, step, half):
    own = step // 2 == 0
    far = step // 2 == 3
    block = jnp.where(own, batch, jnp.where(far, batch + 2, batch + 3 + 2 * half))
    piece = jnp.where(own, 2 * step + half, jnp.where(far, step - 6 + 2 * half, step - 2))
    return lax.rem(block, 4) * 4 + piece


def slot_of(batch, group):
    away = lax.rem(group // 4 + 4 - batch, 4)
    piece = lax.rem(group, 4)
    near = 4 + 2 * piece + jnp.where(away == 1, 1, 0)
    far = 12 + 2 * lax.rem(piece, 2) + piece // 2
    return jnp.where(away == 0, piece, jnp.where(away == 2, far, near))


def kernel(
    samples, weight, bias, upstream,
    st_out, g_buf, act_out, bias_out,
    st_buf, s_buf, w_buf, bias_buf,
    a_send_buf, a_buf, b_send_buf, b_buf, z_buf, c_buf,
    part, asm, u_buf, u_pair, act_buf,
    load_sem, w_sem, bias_sem, u_sem, y_send, y_recv, us_sem, ur_sem, uz_send, uz_recv,
    a_send, a_recv, b_send, b_recv, z_send, z_recv, c_send, c_recv, st_sem,
):
    y_lo, z, x, core = (lax.axis_index(name) for name in SENSOR)
    batch = lax.axis_index("batch")
    mine = 2 * x + core
    up, down = lax.rem(batch + 1, 4), lax.rem(batch + 3, 4)
    other = 1 - y_lo

    def class_peer(d):
        k = lax.rem(mine + d, CLASSES)
        return k, {"x": k // 2, "core": lax.rem(k, 2)}

    def z_peer(d):
        return {"z": lax.rem(z + d, DEPTH)}

    loads = [
        pltpu.make_async_copy(samples.at[pl.ds(PIECE * i, PIECE)], s_buf.at[i], load_sem.at[i]) for i in range(8)
    ]
    load_u = pltpu.make_async_copy(upstream, u_buf.at[z, y_lo], u_sem)
    load_w = pltpu.make_async_copy(weight, w_buf, w_sem)
    load_bias = pltpu.make_async_copy(bias, bias_buf, bias_sem)
    load_u.start()
    for copy in loads:
        copy.start()
    load_bias.start()
    load_w.start()

    barrier = pltpu.get_barrier_semaphore()
    for peer in (up, down):
        pl.semaphore_signal(barrier, inc=1, device_id={"batch": peer})
    pl.semaphore_signal(barrier, inc=1, device_id={"y_lo": other})
    for d in range(1, CLASSES):
        pl.semaphore_signal(barrier, inc=1, device_id=class_peer(d)[1])
    for d in range(1, DEPTH):
        pl.semaphore_signal(barrier, inc=1, device_id=z_peer(d))
    load_u.wait()
    for copy in loads:
        copy.wait()
    pl.semaphore_wait(barrier, 3 + CLASSES - 1 + DEPTH - 1)

    u_cross = pltpu.make_async_remote_copy(
        src_ref=u_buf.at[z, y_lo], dst_ref=u_buf.at[z, y_lo], send_sem=us_sem, recv_sem=ur_sem,
        device_id={"y_lo": other},
    )
    u_cross.start()

    def landing(i, direction):
        return 8 + 4 * (i // 2) + 2 * direction + i % 2

    def y_copy(i, direction):
        source = i if i < 8 else landing(i - 8 + 4 * direction, direction)
        target = landing(i, direction)
        return pltpu.make_async_remote_copy(
            src_ref=s_buf.at[source],
            dst_ref=s_buf.at[target],
            send_sem=y_send.at[direction, i],
            recv_sem=y_recv.at[target],
            device_id={"batch": up if direction == 0 else down},
        )

    def y_start(i):
        for direction in range(2):
            y_copy(i, direction).start()

    def y_arrive(i):
        for direction in range(2):
            y_copy(i, direction).wait_recv()
        if i + AHEAD < 12:
            y_start(i + AHEAD)

    for i in range(AHEAD):
        y_start(i)
    load_bias.wait()
    load_w.wait()

    def spread(source, target, send_sem, recv_sem, peers):
        for device in peers:
            pltpu.make_async_remote_copy(
                src_ref=source, dst_ref=target, send_sem=send_sem, recv_sem=recv_sem, device_id=device
            ).start()

    def await_bytes(region, sem):
        pltpu.make_async_copy(region, region, sem).wait()

    def stage_matmul(p):
        rows = s_buf[pl.ds(4 * p, 4)].reshape(2 * ROWS, s_buf.shape[-1])
        part[...] = jnp.dot(rows, w_buf[...], preferred_element_type=jnp.float32)
        for half in range(2):
            for k in range(CLASSES):
                a_send_buf[p, k, OWNED * half : OWNED * (half + 1), :] = part[
                    ROWS * half + OWNED * k : ROWS * half + OWNED * (k + 1), :
                ]
        for d in range(1, CLASSES):
            k, device = class_peer(d)
            spread(a_send_buf.at[p, k], a_buf.at[p, mine], a_send.at[p], a_recv.at[p], [device])

    def stage_class_sum(p):
        await_bytes(a_buf.at[p, pl.ds(0, CLASSES - 1)], a_recv.at[p])
        total = a_send_buf[p, mine]
        for d in range(1, CLASSES):
            total = total + a_buf[p, lax.rem(mine + d, CLASSES)]
        b_send_buf[p] = total
        spread(b_send_buf.at[p], b_buf.at[p], b_send.at[p], b_recv.at[p], [{"y_lo": other}])

    def stage_pair_sum(p):
        await_bytes(b_buf.at[p], b_recv.at[p])
        z_buf[p, z] = b_send_buf[p] + b_buf[p]
        spread(z_buf.at[p, z], z_buf.at[p, z], z_send.at[p], z_recv.at[p], [z_peer(d) for d in range(1, DEPTH)])

    def stage_gradient(p):
        await_bytes(z_buf.at[p, pl.ds(0, DEPTH - 1)], z_recv.at[p])
        total = z_buf[p, 0]
        for i in range(1, DEPTH):
            total = total + z_buf[p, i]
        act = jnp.tanh(total + bias_buf[...][None, :])
        for half in range(2):
            group = group_of(batch, p, half)
            rows = slice(OWNED * half, OWNED * (half + 1))
            u_pair[rows, :] = u_buf[lax.rem(group, DEPTH), group // DEPTH].astype(jnp.float32)
            act_buf[2 * p + half] = act[rows]
        grad = (u_pair[...] * (1.0 - act * act)).astype(jnp.bfloat16).astype(jnp.float32)
        c_buf[p, mine] = grad
        spread(
            c_buf.at[p, mine], c_buf.at[p, mine], c_send.at[p], c_recv.at[p],
            [class_peer(d)[1] for d in range(1, CLASSES)],
        )

    def stage_assemble(p):
        await_bytes(c_buf.at[p, pl.ds(0, CLASSES - 1)], c_recv.at[p])
        for half in range(2):
            for k in range(CLASSES):
                asm[ROWS * half + OWNED * k : ROWS * half + OWNED * (k + 1), :] = c_buf[
                    p, k, OWNED * half : OWNED * (half + 1), :
                ]
        grads = asm[...]
        g_buf[pl.ds(pl.multiple_of(2 * ROWS * p, 2 * ROWS), 2 * ROWS)] = grads.astype(jnp.bfloat16)
        bias_out[...] += jnp.sum(grads, axis=0, keepdims=True)

    def st_copy(block):
        return pltpu.make_async_copy(st_buf.at[block], st_out.at[block], st_sem.at[block])

    def turn(block):
        rows = s_buf[8 * block : 8 * block + 8].reshape(4 * ROWS, s_buf.shape[-1])
        st_buf[block] = rows.T
        st_copy(block).start()

    bias_out[...] = jnp.zeros_like(bias_out)

    def wave(s):
        if 2 <= s < STEPS:
            y_arrive(2 * s - 4)
        if 0 <= s - 5 < STEPS - 2:
            stage_assemble(s - 5)
        if 0 <= s - 4 < STEPS - 2:
            stage_gradient(s - 4)
        if 2 <= s < STEPS:
            y_arrive(2 * s - 3)
        if s < STEPS:
            stage_matmul(s)
        if s == STEPS - 1:
            turn(3)
        if 0 <= s - 3 < STEPS - 2:
            stage_pair_sum(s - 3)
        if 0 <= s - 1 < STEPS:
            stage_class_sum(s - 1)

    wave(0)
    u_cross.wait()
    spread(u_buf.at[z], u_buf.at[z], uz_send, uz_recv, [z_peer(d) for d in range(1, DEPTH)])
    wave(1)
    turn(0)
    wave(2)
    wave(3)
    turn(1)
    await_bytes(u_buf.at[pl.ds(0, DEPTH - 1)], uz_recv)
    wave(4)
    wave(5)
    turn(2)
    wave(6)
    wave(7)
    wave(8)
    last = (STEPS - 2, STEPS - 1)
    for stage in (stage_pair_sum, stage_gradient, stage_assemble):
        if stage is stage_pair_sum:
            wave(9)
        for p in last:
            stage(p)
        if stage is stage_pair_sum:
            wave(10)

    act_out[...] = act_buf[slot_of(batch, y_lo * DEPTH + z)]

    for direction in range(2):
        for i in range(12):
            y_copy(i, direction).wait_send()
    await_bytes(u_buf.at[pl.ds(0, DEPTH - 1)], uz_send)
    for block in range(4):
        st_copy(block).wait()

    @pl.loop(0, STEPS)
    def _(p):
        await_bytes(a_buf.at[p, pl.ds(0, CLASSES - 1)], a_send.at[p])
        await_bytes(b_buf.at[p], b_send.at[p])
        await_bytes(z_buf.at[p, pl.ds(0, DEPTH - 1)], z_send.at[p])
        await_bytes(c_buf.at[p, pl.ds(0, CLASSES - 1)], c_send.at[p])


def weight_kernel(st, g, act, bias, grad_out, act_out, bias_out):
    rows = jnp.concatenate([st[block] for block in range(4)], axis=1)
    grad_out[...] = jnp.dot(rows, g[...], preferred_element_type=jnp.float32).astype(jnp.bfloat16)
    act_out[...] = act[...].astype(jnp.bfloat16)
    bias_out[...] = bias[0]


def body(samples, branch_weight, branch_bias, upstream):
    sensors, hidden = branch_weight.shape
    funcs = 4 * samples.shape[0]
    share = 2 * OWNED
    f32, bf16 = jnp.float32, jnp.bfloat16
    dma = pltpu.SemaphoreType.DMA
    turned, grads, act, bias_sum = pl.pallas_call(
        kernel,
        out_shape=(
            jax.ShapeDtypeStruct((4, sensors, funcs // 4), bf16),
            jax.ShapeDtypeStruct((funcs, hidden), bf16),
            jax.ShapeDtypeStruct((OWNED, hidden), f32),
            jax.ShapeDtypeStruct((1, hidden), f32),
        ),
        in_specs=[pl.BlockSpec(memory_space=pl.ANY)] * 4,
        out_specs=(pl.BlockSpec(memory_space=pl.ANY), *[pl.BlockSpec(memory_space=pltpu.VMEM)] * 3),
        scratch_shapes=[
            pltpu.VMEM((4, sensors, funcs // 4), bf16),
            pltpu.VMEM((32, PIECE, sensors), bf16),
            pltpu.VMEM((sensors, hidden), bf16),
            pltpu.VMEM((hidden,), f32),
            pltpu.VMEM((STEPS, CLASSES, share, hidden), f32),
            pltpu.VMEM((STEPS, CLASSES, share, hidden), f32),
            pltpu.VMEM((STEPS, share, hidden), f32),
            pltpu.VMEM((STEPS, share, hidden), f32),
            pltpu.VMEM((STEPS, DEPTH, share, hidden), f32),
            pltpu.VMEM((STEPS, CLASSES, share, hidden), f32),
            pltpu.VMEM((2 * ROWS, hidden), f32),
            pltpu.VMEM((2 * ROWS, hidden), f32),
            pltpu.VMEM((DEPTH, 2, OWNED, hidden), bf16),
            pltpu.VMEM((share, hidden), f32),
            pltpu.VMEM((2 * STEPS, OWNED, hidden), f32),
            dma((8,)), dma, dma, dma, dma((2, 12)), dma((32,)), dma, dma, dma, dma,
            dma((STEPS,)), dma((STEPS,)), dma((STEPS,)), dma((STEPS,)),
            dma((STEPS,)), dma((STEPS,)), dma((STEPS,)), dma((STEPS,)),
            dma((4,)),
        ],
        compiler_params=pltpu.CompilerParams(
            collective_id=0, has_side_effects=True, vmem_limit_bytes=63 * 1024 * 1024
        ),
    )(samples, branch_weight, branch_bias, upstream)
    whole = lambda *shape: pl.BlockSpec(shape, lambda t: (0,) * len(shape))
    weight_grad, activation, bias_grad = pl.pallas_call(
        weight_kernel,
        grid=(sensors // TILE,),
        out_shape=(
            jax.ShapeDtypeStruct((sensors, hidden), bf16),
            jax.ShapeDtypeStruct((OWNED, hidden), bf16),
            jax.ShapeDtypeStruct((hidden,), f32),
        ),
        in_specs=[pl.BlockSpec((4, TILE, funcs // 4), lambda t: (0, t, 0)), whole(funcs, hidden), whole(OWNED, hidden), whole(1, hidden)],
        out_specs=(pl.BlockSpec((TILE, hidden), lambda t: (t, 0)), whole(OWNED, hidden), whole(hidden)),
    )(turned, grads, act, bias_sum)
    return activation, weight_grad, bias_grad


def solution(mesh):
    torus = Mesh(
        mesh.devices.reshape(2, 8, 4, 2, mesh.shape["batch"]),
        (*SENSOR, "batch"),
    )
    in_specs = (P("batch", SENSOR), P(SENSOR, "batch"), P("batch"), P(SENSOR, "batch"))
    out_specs = (P(SENSOR, "batch"), P(SENSOR, "batch"), P("batch"))
    return jax.shard_map(body, mesh=torus, in_specs=in_specs, out_specs=out_specs, check_vma=False)
```

```python
import jax
import jax.numpy as jnp
from jax import lax
from jax.experimental import pallas as pl
from jax.experimental.pallas import tpu as pltpu
from jax.sharding import Mesh
from jax.sharding import PartitionSpec as P

SENSOR = ("y_lo", "z", "x", "core")
STEPS = 10
WIDE = 6
ROWS = 32
PIECE = 16
PIECES = 12
AHEAD = 3
OWNED = 4
CLASSES = 8
DEPTH = 8
TILE = 1024
JOINED = (8, 9)


def halves(p):
    return 2 if p < WIDE else 1


def group_of(batch, p, half):
    if p < 2:
        return batch * 4 + 2 * p + half
    if p < WIDE:
        return lax.rem(batch + 3 + 2 * half, 4) * 4 + p - 2
    return lax.rem(batch + 2, 4) * 4 + p - WIDE


def slot_of(batch, group):
    away = lax.rem(group // 4 + 4 - batch, 4)
    piece = lax.rem(group, 4)
    near = 4 + 2 * piece + jnp.where(away == 1, 1, 0)
    return jnp.where(away == 0, piece, jnp.where(away == 2, 12 + piece, near))


def kernel(
    samples, weight, bias, upstream,
    st_out, g_buf, act_out, bias_out,
    st_buf, s_buf, w_buf, bias_buf,
    a_send_w, a_w, b_send_w, b_w, z_w, c_w,
    a_send_t, a_t, b_send_t, b_t, z_t, c_t,
    part, asm, u_buf, u_pair, act_buf,
    load_sem, w_sem, bias_sem, u_sem, y_send, y_recv, us_sem, ur_sem, uz_send, uz_recv,
    a_send, a_recv, b_send, b_recv, z_send, z_recv, c_send, c_recv, st_sem,
):
    y_lo, z, x, core = (lax.axis_index(name) for name in SENSOR)
    batch = lax.axis_index("batch")
    mine = 2 * x + core
    up, down = lax.rem(batch + 1, 4), lax.rem(batch + 3, 4)
    other = 1 - y_lo

    def class_peer(d):
        k = lax.rem(mine + d, CLASSES)
        return k, {"x": k // 2, "core": lax.rem(k, 2)}

    def z_peer(d):
        return {"z": lax.rem(z + d, DEPTH)}

    place = DEPTH * y_lo + z

    def place_peer(d):
        there = lax.rem(place + d, 2 * DEPTH)
        return {"y_lo": there // DEPTH, "z": lax.rem(there, DEPTH)}

    class_peers = [class_peer(d)[1] for d in range(1, CLASSES)]
    z_peers = [z_peer(d) for d in range(1, DEPTH)]
    place_peers = [place_peer(d) for d in range(1, 2 * DEPTH)]

    loads = [
        pltpu.make_async_copy(samples.at[pl.ds(PIECE * i, PIECE)], s_buf.at[i], load_sem.at[i]) for i in range(8)
    ]
    load_u = pltpu.make_async_copy(upstream, u_buf.at[z, y_lo], u_sem)
    load_w = pltpu.make_async_copy(weight, w_buf, w_sem)
    load_bias = pltpu.make_async_copy(bias, bias_buf, bias_sem)
    load_u.start()
    for copy in loads:
        copy.start()
    load_bias.start()
    load_w.start()

    barrier = pltpu.get_barrier_semaphore()
    for peer in (up, down):
        pl.semaphore_signal(barrier, inc=1, device_id={"batch": peer})
    for device in class_peers + place_peers:
        pl.semaphore_signal(barrier, inc=1, device_id=device)
    load_u.wait()
    for copy in loads:
        copy.wait()
    pl.semaphore_wait(barrier, 2 + CLASSES - 1 + 2 * DEPTH - 1)

    u_cross = pltpu.make_async_remote_copy(
        src_ref=u_buf.at[z, y_lo], dst_ref=u_buf.at[z, y_lo], send_sem=us_sem, recv_sem=ur_sem,
        device_id={"y_lo": other},
    )
    u_cross.start()

    def landing(i, direction):
        return 8 + 4 * (i // 2) + 2 * direction + i % 2 if i < 8 else 24 + 2 * (i - 8) + direction

    def y_copy(i, direction):
        source = i if i < 8 else landing(2 * (i - 8) + direction, direction)
        target = landing(i, direction)
        return pltpu.make_async_remote_copy(
            src_ref=s_buf.at[source],
            dst_ref=s_buf.at[target],
            send_sem=y_send.at[direction, i],
            recv_sem=y_recv.at[target],
            device_id={"batch": up if direction == 0 else down},
        )

    def y_start(i):
        for direction in range(2):
            y_copy(i, direction).start()

    def y_arrive(i):
        for direction in range(2):
            y_copy(i, direction).wait_recv()
        if i + AHEAD < PIECES:
            y_start(i + AHEAD)

    for i in range(AHEAD):
        y_start(i)
    load_bias.wait()
    load_w.wait()

    def spread(source, target, send_sem, recv_sem, peers):
        for device in peers:
            pltpu.make_async_remote_copy(
                src_ref=source, dst_ref=target, send_sem=send_sem, recv_sem=recv_sem, device_id=device
            ).start()

    def await_bytes(region, sem):
        pltpu.make_async_copy(region, region, sem).wait()

    def of(wide, thin, p):
        return wide.at[p] if p < WIDE else thin.at[p - WIDE]

    def stage_matmul(p):
        first, count = (4 * p, 4) if p < WIDE else (24 + 2 * (p - WIDE), 2)
        rows = s_buf[first : first + count].reshape(count * PIECE, s_buf.shape[-1])
        part[: count * PIECE] = jnp.dot(rows, w_buf[...], preferred_element_type=jnp.float32)
        outgoing = of(a_send_w, a_send_t, p)
        for half in range(halves(p)):
            for k in range(CLASSES):
                outgoing[k, OWNED * half : OWNED * (half + 1), :] = part[
                    ROWS * half + OWNED * k : ROWS * half + OWNED * (k + 1), :
                ]
        for d in range(1, CLASSES):
            k, device = class_peer(d)
            spread(outgoing.at[k], of(a_w, a_t, p).at[mine], a_send.at[p], a_recv.at[p], [device])

    def stage_class_sum(p):
        incoming = of(a_w, a_t, p)
        await_bytes(incoming.at[pl.ds(0, CLASSES - 1)], a_recv.at[p])
        total = of(a_send_w, a_send_t, p)[mine]
        for d in range(1, CLASSES):
            total = total + incoming[lax.rem(mine + d, CLASSES)]
        total = total.astype(jnp.bfloat16)
        if p in JOINED:
            shares = of(z_w, z_t, p)
            shares[place] = total
            spread(shares.at[place], shares.at[place], z_send.at[p], z_recv.at[p], place_peers)
        else:
            outgoing = of(b_send_w, b_send_t, p)
            outgoing[...] = total
            spread(outgoing, of(b_w, b_t, p), b_send.at[p], b_recv.at[p], [{"y_lo": other}])

    def stage_pair_sum(p):
        incoming = of(b_w, b_t, p)
        await_bytes(incoming, b_recv.at[p])
        total = of(b_send_w, b_send_t, p)[...].astype(jnp.float32) + incoming[...].astype(jnp.float32)
        shares = of(z_w, z_t, p)
        shares[z] = total.astype(jnp.bfloat16)
        spread(shares.at[z], shares.at[z], z_send.at[p], z_recv.at[p], z_peers)

    def stage_gradient(p):
        shares = of(z_w, z_t, p)
        count = 2 * DEPTH if p in JOINED else DEPTH
        await_bytes(shares.at[pl.ds(0, count - 1)], z_recv.at[p])
        total = shares[0].astype(jnp.float32)
        for i in range(1, count):
            total = total + shares[i].astype(jnp.float32)
        act = jnp.tanh(total + bias_buf[...][None, :])
        for half in range(halves(p)):
            group = group_of(batch, p, half)
            rows = slice(OWNED * half, OWNED * (half + 1))
            u_pair[rows, :] = u_buf[lax.rem(group, DEPTH), group // DEPTH].astype(jnp.float32)
            act_buf[2 * p + half if p < WIDE else p + WIDE] = act[rows]
        scale = u_pair[: OWNED * halves(p)]
        grads = of(c_w, c_t, p)
        grads[mine] = (scale * (1.0 - act * act)).astype(jnp.bfloat16)
        spread(grads.at[mine], grads.at[mine], c_send.at[p], c_recv.at[p], class_peers)

    def stage_assemble(p):
        incoming = of(c_w, c_t, p)
        await_bytes(incoming.at[pl.ds(0, CLASSES - 1)], c_recv.at[p])
        for k in range(CLASSES):
            grads = incoming[k].astype(jnp.float32)
            for half in range(halves(p)):
                asm[ROWS * half + OWNED * k : ROWS * half + OWNED * (k + 1), :] = grads[
                    OWNED * half : OWNED * (half + 1)
                ]
        size = ROWS * halves(p)
        first = 2 * ROWS * p if p < WIDE else ROWS * (p + WIDE)
        grads = asm[:size]
        g_buf[first : first + size] = grads.astype(jnp.bfloat16)
        bias_out[...] += jnp.sum(grads, axis=0, keepdims=True)

    def st_copy(block):
        return pltpu.make_async_copy(st_buf.at[block], st_out.at[block], st_sem.at[block])

    def turn(block):
        rows = s_buf[8 * block : 8 * block + 8].reshape(4 * ROWS, s_buf.shape[-1])
        st_buf[block] = rows.T
        st_copy(block).start()

    bias_out[...] = jnp.zeros_like(bias_out)

    matmul, class_sum, pair_sum, gradient, assemble = (
        stage_matmul, stage_class_sum, stage_pair_sum, stage_gradient, stage_assemble
    )

    matmul(0)
    matmul(1)
    y_arrive(0)
    u_cross.wait()
    spread(u_buf.at[z], u_buf.at[z], uz_send, uz_recv, z_peers)
    y_arrive(1)
    matmul(2)
    class_sum(0)
    class_sum(1)
    y_arrive(2)
    turn(0)
    y_arrive(3)
    matmul(3)
    class_sum(2)
    y_arrive(4)
    pair_sum(0)
    y_arrive(5)
    matmul(4)
    pair_sum(1)
    class_sum(3)
    y_arrive(6)
    pair_sum(2)
    await_bytes(u_buf.at[pl.ds(0, DEPTH - 1)], uz_recv)
    y_arrive(7)
    matmul(5)
    gradient(0)
    class_sum(4)
    turn(1)
    y_arrive(8)
    matmul(6)
    gradient(1)
    pair_sum(3)
    class_sum(5)
    y_arrive(9)
    matmul(7)
    gradient(2)
    assemble(0)
    turn(2)
    class_sum(6)
    y_arrive(10)
    matmul(8)
    pair_sum(4)
    assemble(1)
    class_sum(7)
    y_arrive(11)
    matmul(9)
    pair_sum(5)
    pair_sum(6)
    gradient(3)
    assemble(2)
    class_sum(8)
    pair_sum(7)
    gradient(4)
    turn(3)
    class_sum(9)
    assemble(3)
    gradient(5)
    gradient(6)
    gradient(7)
    gradient(8)
    assemble(4)
    assemble(5)
    gradient(9)
    assemble(6)
    assemble(7)
    assemble(8)
    assemble(9)

    act_out[...] = act_buf[slot_of(batch, y_lo * DEPTH + z)]

    for direction in range(2):
        for i in range(PIECES):
            y_copy(i, direction).wait_send()
    await_bytes(u_buf.at[pl.ds(0, DEPTH - 1)], uz_send)
    for p in range(STEPS):
        await_bytes(of(a_w, a_t, p).at[pl.ds(0, CLASSES - 1)], a_send.at[p])
        if p not in JOINED:
            await_bytes(of(b_w, b_t, p), b_send.at[p])
        count = 2 * DEPTH if p in JOINED else DEPTH
        await_bytes(of(z_w, z_t, p).at[pl.ds(0, count - 1)], z_send.at[p])
        await_bytes(of(c_w, c_t, p).at[pl.ds(0, CLASSES - 1)], c_send.at[p])
    for block in range(4):
        st_copy(block).wait()


def weight_kernel(st, g, act, bias, grad_out, act_out, bias_out):
    rows = jnp.concatenate([st[block] for block in range(4)], axis=1)
    grad_out[...] = jnp.dot(rows, g[...], preferred_element_type=jnp.float32).astype(jnp.bfloat16)
    act_out[...] = act[...].astype(jnp.bfloat16)
    bias_out[...] = bias[0]


def exchange_buffers(steps, rows, places, hidden):
    f32, bf16 = jnp.float32, jnp.bfloat16
    return [
        pltpu.VMEM((steps, CLASSES, rows, hidden), f32),
        pltpu.VMEM((steps, CLASSES, rows, hidden), f32),
        pltpu.VMEM((steps, rows, hidden), bf16),
        pltpu.VMEM((steps, rows, hidden), bf16),
        pltpu.VMEM((steps, places, rows, hidden), bf16),
        pltpu.VMEM((steps, CLASSES, rows, hidden), bf16),
    ]


def body(samples, branch_weight, branch_bias, upstream):
    sensors, hidden = branch_weight.shape
    funcs = 4 * samples.shape[0]
    f32, bf16 = jnp.float32, jnp.bfloat16
    dma = pltpu.SemaphoreType.DMA
    turned, grads, act, bias_sum = pl.pallas_call(
        kernel,
        out_shape=(
            jax.ShapeDtypeStruct((4, sensors, funcs // 4), bf16),
            jax.ShapeDtypeStruct((funcs, hidden), bf16),
            jax.ShapeDtypeStruct((OWNED, hidden), f32),
            jax.ShapeDtypeStruct((1, hidden), f32),
        ),
        in_specs=[pl.BlockSpec(memory_space=pl.ANY)] * 4,
        out_specs=(pl.BlockSpec(memory_space=pl.ANY), *[pl.BlockSpec(memory_space=pltpu.VMEM)] * 3),
        scratch_shapes=[
            pltpu.VMEM((4, sensors, funcs // 4), bf16),
            pltpu.VMEM((32, PIECE, sensors), bf16),
            pltpu.VMEM((sensors, hidden), bf16),
            pltpu.VMEM((hidden,), f32),
            *exchange_buffers(WIDE, 2 * OWNED, DEPTH, hidden),
            *exchange_buffers(STEPS - WIDE, OWNED, 2 * DEPTH, hidden),
            pltpu.VMEM((2 * ROWS, hidden), f32),
            pltpu.VMEM((2 * ROWS, hidden), f32),
            pltpu.VMEM((DEPTH, 2, OWNED, hidden), bf16),
            pltpu.VMEM((2 * OWNED, hidden), f32),
            pltpu.VMEM((16, OWNED, hidden), f32),
            dma((8,)), dma, dma, dma, dma((2, PIECES)), dma((32,)), dma, dma, dma, dma,
            dma((STEPS,)), dma((STEPS,)), dma((STEPS,)), dma((STEPS,)),
            dma((STEPS,)), dma((STEPS,)), dma((STEPS,)), dma((STEPS,)),
            dma((4,)),
        ],
        compiler_params=pltpu.CompilerParams(
            collective_id=0, has_side_effects=True, vmem_limit_bytes=63 * 1024 * 1024
        ),
    )(samples, branch_weight, branch_bias, upstream)
    whole = lambda *shape: pl.BlockSpec(shape, lambda t: (0,) * len(shape))
    weight_grad, activation, bias_grad = pl.pallas_call(
        weight_kernel,
        grid=(sensors // TILE,),
        out_shape=(
            jax.ShapeDtypeStruct((sensors, hidden), bf16),
            jax.ShapeDtypeStruct((OWNED, hidden), bf16),
            jax.ShapeDtypeStruct((hidden,), f32),
        ),
        in_specs=[pl.BlockSpec((4, TILE, funcs // 4), lambda t: (0, t, 0)), whole(funcs, hidden), whole(OWNED, hidden), whole(1, hidden)],
        out_specs=(pl.BlockSpec((TILE, hidden), lambda t: (t, 0)), whole(OWNED, hidden), whole(hidden)),
    )(turned, grads, act, bias_sum)
    return activation, weight_grad, bias_grad


def solution(mesh):
    torus = Mesh(
        mesh.devices.reshape(2, 8, 4, 2, mesh.shape["batch"]),
        (*SENSOR, "batch"),
    )
    in_specs = (P("batch", SENSOR), P(SENSOR, "batch"), P("batch"), P(SENSOR, "batch"))
    out_specs = (P(SENSOR, "batch"), P(SENSOR, "batch"), P("batch"))
    return jax.shard_map(body, mesh=torus, in_specs=in_specs, out_specs=out_specs, check_vma=False)
```

```python
import jax
import jax.numpy as jnp
from jax import lax
from jax.experimental import pallas as pl
from jax.experimental.pallas import tpu as pltpu
from jax.sharding import Mesh
from jax.sharding import PartitionSpec as P

SENSOR = ("y_lo", "z", "x", "core")
STEPS = 10
WIDE = 6
ROWS = 32
PIECE = 16
PIECES = 12
AHEAD = 3
OWNED = 4
CLASSES = 8
DEPTH = 8
TILE = 1024
JOINED = (8, 9)


def halves(p):
    return 2 if p < WIDE else 1


def group_of(batch, p, half):
    if p < 2:
        return batch * 4 + 2 * p + half
    if p < WIDE:
        return lax.rem(batch + 3 + 2 * half, 4) * 4 + p - 2
    return lax.rem(batch + 2, 4) * 4 + p - WIDE


def slot_of(batch, group):
    away = lax.rem(group // 4 + 4 - batch, 4)
    piece = lax.rem(group, 4)
    near = 4 + 2 * piece + jnp.where(away == 1, 1, 0)
    return jnp.where(away == 0, piece, jnp.where(away == 2, 12 + piece, near))


def kernel(
    samples, weight, bias, upstream,
    st_out, g_buf, act_out, bias_out,
    st_buf, s_buf, w_buf, bias_buf,
    a_send_w, a_w, b_send_w, b_w, z_w, c_w,
    a_send_t, a_t, b_send_t, b_t, z_t, c_t, joined,
    part, asm, u_buf, u_pair, act_buf,
    load_sem, w_sem, bias_sem, u_sem, y_send, y_recv, us_sem, ur_sem, uz_send, uz_recv,
    a_send, a_recv, b_send, b_recv, z_send, z_recv, c_send, c_recv, st_sem,
):
    y_lo, z, x, core = (lax.axis_index(name) for name in SENSOR)
    batch = lax.axis_index("batch")
    mine = 2 * x + core
    up, down = lax.rem(batch + 1, 4), lax.rem(batch + 3, 4)
    other = 1 - y_lo

    def class_peer(d):
        k = lax.rem(mine + d, CLASSES)
        return k, {"x": k // 2, "core": lax.rem(k, 2)}

    def z_peer(d):
        return {"z": lax.rem(z + d, DEPTH)}

    place = DEPTH * y_lo + z

    def place_peer(d):
        there = lax.rem(place + d, 2 * DEPTH)
        return {"y_lo": there // DEPTH, "z": lax.rem(there, DEPTH)}

    class_peers = [class_peer(d)[1] for d in range(1, CLASSES)]
    z_peers = [z_peer(d) for d in range(1, DEPTH)]
    place_peers = [place_peer(d) for d in range(1, 2 * DEPTH)]

    loads = [
        pltpu.make_async_copy(samples.at[pl.ds(PIECE * i, PIECE)], s_buf.at[i], load_sem.at[i]) for i in range(8)
    ]
    load_u = pltpu.make_async_copy(upstream, u_buf.at[z, y_lo], u_sem)
    load_w = pltpu.make_async_copy(weight, w_buf, w_sem)
    load_bias = pltpu.make_async_copy(bias, bias_buf, bias_sem)
    load_u.start()
    for copy in loads:
        copy.start()
    load_bias.start()
    load_w.start()

    barrier = pltpu.get_barrier_semaphore()
    for peer in (up, down):
        pl.semaphore_signal(barrier, inc=1, device_id={"batch": peer})
    for device in class_peers + place_peers:
        pl.semaphore_signal(barrier, inc=1, device_id=device)
    load_u.wait()
    for copy in loads:
        copy.wait()
    pl.semaphore_wait(barrier, 2 + CLASSES - 1 + 2 * DEPTH - 1)

    u_cross = pltpu.make_async_remote_copy(
        src_ref=u_buf.at[z, y_lo], dst_ref=u_buf.at[z, y_lo], send_sem=us_sem, recv_sem=ur_sem,
        device_id={"y_lo": other},
    )
    u_cross.start()

    def landing(i, direction):
        return 8 + 4 * (i // 2) + 2 * direction + i % 2 if i < 8 else 24 + 2 * (i - 8) + direction

    def y_copy(i, direction):
        source = i if i < 8 else landing(2 * (i - 8) + direction, direction)
        target = landing(i, direction)
        return pltpu.make_async_remote_copy(
            src_ref=s_buf.at[source],
            dst_ref=s_buf.at[target],
            send_sem=y_send.at[direction, i],
            recv_sem=y_recv.at[target],
            device_id={"batch": up if direction == 0 else down},
        )

    def y_start(i):
        for direction in range(2):
            y_copy(i, direction).start()

    def y_arrive(i):
        for direction in range(2):
            y_copy(i, direction).wait_recv()
        if i + AHEAD < PIECES:
            y_start(i + AHEAD)

    for i in range(AHEAD):
        y_start(i)
    load_bias.wait()
    load_w.wait()

    def spread(source, target, send_sem, recv_sem, peers):
        for device in peers:
            pltpu.make_async_remote_copy(
                src_ref=source, dst_ref=target, send_sem=send_sem, recv_sem=recv_sem, device_id=device
            ).start()

    def await_bytes(region, sem):
        pltpu.make_async_copy(region, region, sem).wait()

    def of(wide, thin, p):
        return wide.at[p] if p < WIDE else thin.at[p - WIDE]

    def stage_matmul(p):
        first, count = (4 * p, 4) if p < WIDE else (24 + 2 * (p - WIDE), 2)
        rows = s_buf[first : first + count].reshape(count * PIECE, s_buf.shape[-1])
        part[: count * PIECE] = jnp.dot(rows, w_buf[...], preferred_element_type=jnp.float32)
        outgoing = of(a_send_w, a_send_t, p)
        for half in range(halves(p)):
            for k in range(CLASSES):
                outgoing[k, OWNED * half : OWNED * (half + 1), :] = part[
                    ROWS * half + OWNED * k : ROWS * half + OWNED * (k + 1), :
                ]
        for d in range(1, CLASSES):
            k, device = class_peer(d)
            spread(outgoing.at[k], of(a_w, a_t, p).at[mine], a_send.at[p], a_recv.at[p], [device])

    def stage_class_sum(p):
        incoming = of(a_w, a_t, p)
        await_bytes(incoming.at[pl.ds(0, CLASSES - 1)], a_recv.at[p])
        total = of(a_send_w, a_send_t, p)[mine]
        for d in range(1, CLASSES):
            total = total + incoming[lax.rem(mine + d, CLASSES)]
        if p in JOINED:
            shares = joined.at[p - JOINED[0]]
            shares[place] = total.astype(jnp.bfloat16)
            spread(shares.at[place], shares.at[place], z_send.at[p], z_recv.at[p], place_peers)
        else:
            shares = of(z_w, z_t, p)
            shares[z] = total
            spread(shares.at[z], shares.at[z], z_send.at[p], z_recv.at[p], z_peers)

    def sum_shares(shares, p):
        count = shares.shape[0]
        await_bytes(shares.at[pl.ds(0, count - 1)], z_recv.at[p])
        total = shares[0].astype(jnp.float32)
        for i in range(1, count):
            total = total + shares[i].astype(jnp.float32)
        return total

    def stage_z_sum(p):
        outgoing = of(b_send_w, b_send_t, p)
        outgoing[...] = sum_shares(of(z_w, z_t, p), p).astype(jnp.bfloat16)
        spread(outgoing, of(b_w, b_t, p), b_send.at[p], b_recv.at[p], [{"y_lo": other}])

    def stage_gradient(p):
        if p in JOINED:
            total = sum_shares(joined.at[p - JOINED[0]], p)
        else:
            incoming = of(b_w, b_t, p)
            await_bytes(incoming, b_recv.at[p])
            total = of(b_send_w, b_send_t, p)[...].astype(jnp.float32) + incoming[...].astype(jnp.float32)
        act = jnp.tanh(total + bias_buf[...][None, :])
        for half in range(halves(p)):
            group = group_of(batch, p, half)
            rows = slice(OWNED * half, OWNED * (half + 1))
            u_pair[rows, :] = u_buf[lax.rem(group, DEPTH), group // DEPTH].astype(jnp.float32)
            act_buf[2 * p + half if p < WIDE else p + WIDE] = act[rows]
        scale = u_pair[: OWNED * halves(p)]
        grads = of(c_w, c_t, p)
        grads[mine] = (scale * (1.0 - act * act)).astype(jnp.bfloat16)
        spread(grads.at[mine], grads.at[mine], c_send.at[p], c_recv.at[p], class_peers)

    def stage_assemble(p):
        incoming = of(c_w, c_t, p)
        await_bytes(incoming.at[pl.ds(0, CLASSES - 1)], c_recv.at[p])
        for k in range(CLASSES):
            grads = incoming[k].astype(jnp.float32)
            for half in range(halves(p)):
                asm[ROWS * half + OWNED * k : ROWS * half + OWNED * (k + 1), :] = grads[
                    OWNED * half : OWNED * (half + 1)
                ]
        size = ROWS * halves(p)
        first = 2 * ROWS * p if p < WIDE else ROWS * (p + WIDE)
        grads = asm[:size]
        g_buf[first : first + size] = grads.astype(jnp.bfloat16)
        bias_out[...] += jnp.sum(grads, axis=0, keepdims=True)

    def st_copy(block):
        return pltpu.make_async_copy(st_buf.at[block], st_out.at[block], st_sem.at[block])

    def turn(block):
        rows = s_buf[8 * block : 8 * block + 8].reshape(4 * ROWS, s_buf.shape[-1])
        st_buf[block] = rows.T
        st_copy(block).start()

    bias_out[...] = jnp.zeros_like(bias_out)

    matmul, class_sum, z_sum, gradient, assemble = (
        stage_matmul, stage_class_sum, stage_z_sum, stage_gradient, stage_assemble
    )

    matmul(0)
    matmul(1)
    y_arrive(0)
    u_cross.wait()
    spread(u_buf.at[z], u_buf.at[z], uz_send, uz_recv, z_peers)
    y_arrive(1)
    matmul(2)
    class_sum(0)
    class_sum(1)
    y_arrive(2)
    turn(0)
    y_arrive(3)
    matmul(3)
    class_sum(2)
    y_arrive(4)
    z_sum(0)
    y_arrive(5)
    matmul(4)
    z_sum(1)
    class_sum(3)
    y_arrive(6)
    z_sum(2)
    turn(1)
    await_bytes(u_buf.at[pl.ds(0, DEPTH - 1)], uz_recv)
    y_arrive(7)
    matmul(5)
    class_sum(4)
    gradient(0)
    y_arrive(8)
    matmul(6)
    z_sum(3)
    gradient(1)
    y_arrive(9)
    matmul(7)
    class_sum(5)
    assemble(0)
    gradient(2)
    class_sum(6)
    y_arrive(10)
    matmul(8)
    z_sum(4)
    assemble(1)
    turn(2)
    class_sum(7)
    y_arrive(11)
    matmul(9)
    gradient(3)
    z_sum(5)
    class_sum(8)
    z_sum(6)
    assemble(2)
    gradient(4)
    turn(3)
    class_sum(9)
    z_sum(7)
    gradient(5)
    gradient(6)
    assemble(3)
    gradient(7)
    gradient(8)
    assemble(4)
    assemble(5)
    gradient(9)
    assemble(6)
    assemble(7)
    assemble(8)
    assemble(9)

    act_out[...] = act_buf[slot_of(batch, y_lo * DEPTH + z)]

    for direction in range(2):
        for i in range(PIECES):
            y_copy(i, direction).wait_send()
    await_bytes(u_buf.at[pl.ds(0, DEPTH - 1)], uz_send)
    for p in range(STEPS):
        await_bytes(of(a_w, a_t, p).at[pl.ds(0, CLASSES - 1)], a_send.at[p])
        if p in JOINED:
            await_bytes(joined.at[p - JOINED[0], pl.ds(0, 2 * DEPTH - 1)], z_send.at[p])
        else:
            await_bytes(of(z_w, z_t, p).at[pl.ds(0, DEPTH - 1)], z_send.at[p])
            await_bytes(of(b_w, b_t, p), b_send.at[p])
        await_bytes(of(c_w, c_t, p).at[pl.ds(0, CLASSES - 1)], c_send.at[p])
    for block in range(4):
        st_copy(block).wait()


def weight_kernel(st, g, act, bias, grad_out, act_out, bias_out):
    rows = jnp.concatenate([st[block] for block in range(4)], axis=1)
    grad_out[...] = jnp.dot(rows, g[...], preferred_element_type=jnp.float32).astype(jnp.bfloat16)
    act_out[...] = act[...].astype(jnp.bfloat16)
    bias_out[...] = bias[0]


def exchange_buffers(steps, rows, hidden):
    f32, bf16 = jnp.float32, jnp.bfloat16
    return [
        pltpu.VMEM((steps, CLASSES, rows, hidden), f32),
        pltpu.VMEM((steps, CLASSES, rows, hidden), f32),
        pltpu.VMEM((steps, rows, hidden), bf16),
        pltpu.VMEM((steps, rows, hidden), bf16),
        pltpu.VMEM((steps, DEPTH, rows, hidden), f32),
        pltpu.VMEM((steps, CLASSES, rows, hidden), bf16),
    ]


def body(samples, branch_weight, branch_bias, upstream):
    sensors, hidden = branch_weight.shape
    funcs = 4 * samples.shape[0]
    f32, bf16 = jnp.float32, jnp.bfloat16
    dma = pltpu.SemaphoreType.DMA
    turned, grads, act, bias_sum = pl.pallas_call(
        kernel,
        out_shape=(
            jax.ShapeDtypeStruct((4, sensors, funcs // 4), bf16),
            jax.ShapeDtypeStruct((funcs, hidden), bf16),
            jax.ShapeDtypeStruct((OWNED, hidden), f32),
            jax.ShapeDtypeStruct((1, hidden), f32),
        ),
        in_specs=[pl.BlockSpec(memory_space=pl.ANY)] * 4,
        out_specs=(pl.BlockSpec(memory_space=pl.ANY), *[pl.BlockSpec(memory_space=pltpu.VMEM)] * 3),
        scratch_shapes=[
            pltpu.VMEM((4, sensors, funcs // 4), bf16),
            pltpu.VMEM((32, PIECE, sensors), bf16),
            pltpu.VMEM((sensors, hidden), bf16),
            pltpu.VMEM((hidden,), f32),
            *exchange_buffers(WIDE, 2 * OWNED, hidden),
            *exchange_buffers(STEPS - WIDE, OWNED, hidden),
            pltpu.VMEM((len(JOINED), 2 * DEPTH, OWNED, hidden), bf16),
            pltpu.VMEM((2 * ROWS, hidden), f32),
            pltpu.VMEM((2 * ROWS, hidden), f32),
            pltpu.VMEM((DEPTH, 2, OWNED, hidden), bf16),
            pltpu.VMEM((2 * OWNED, hidden), f32),
            pltpu.VMEM((16, OWNED, hidden), f32),
            dma((8,)), dma, dma, dma, dma((2, PIECES)), dma((32,)), dma, dma, dma, dma,
            dma((STEPS,)), dma((STEPS,)), dma((STEPS,)), dma((STEPS,)),
            dma((STEPS,)), dma((STEPS,)), dma((STEPS,)), dma((STEPS,)),
            dma((4,)),
        ],
        compiler_params=pltpu.CompilerParams(
            collective_id=0, has_side_effects=True, vmem_limit_bytes=63 * 1024 * 1024
        ),
    )(samples, branch_weight, branch_bias, upstream)
    whole = lambda *shape: pl.BlockSpec(shape, lambda t: (0,) * len(shape))
    weight_grad, activation, bias_grad = pl.pallas_call(
        weight_kernel,
        grid=(sensors // TILE,),
        out_shape=(
            jax.ShapeDtypeStruct((sensors, hidden), bf16),
            jax.ShapeDtypeStruct((OWNED, hidden), bf16),
            jax.ShapeDtypeStruct((hidden,), f32),
        ),
        in_specs=[pl.BlockSpec((4, TILE, funcs // 4), lambda t: (0, t, 0)), whole(funcs, hidden), whole(OWNED, hidden), whole(1, hidden)],
        out_specs=(pl.BlockSpec((TILE, hidden), lambda t: (t, 0)), whole(OWNED, hidden), whole(hidden)),
    )(turned, grads, act, bias_sum)
    return activation, weight_grad, bias_grad


def solution(mesh):
    torus = Mesh(
        mesh.devices.reshape(2, 8, 4, 2, mesh.shape["batch"]),
        (*SENSOR, "batch"),
    )
    in_specs = (P("batch", SENSOR), P(SENSOR, "batch"), P("batch"), P(SENSOR, "batch"))
    out_specs = (P(SENSOR, "batch"), P(SENSOR, "batch"), P("batch"))
    return jax.shard_map(body, mesh=torus, in_specs=in_specs, out_specs=out_specs, check_vma=False)
```

```python
import jax
import jax.numpy as jnp
from jax import lax
from jax.experimental import pallas as pl
from jax.experimental.pallas import tpu as pltpu
from jax.sharding import Mesh
from jax.sharding import PartitionSpec as P

SENSOR = ("y_lo", "z", "x", "core")
STEPS = 10
WIDE = 6
ROWS = 32
PIECE = 16
PIECES = 12
AHEAD = 3
OWNED = 4
CLASSES = 8
DEPTH = 8
TILE = 1024
JOINED = (8, 9)


def halves(p):
    return 2 if p < WIDE else 1


def group_of(batch, p, half):
    if p < 2:
        return batch * 4 + 2 * p + half
    if p < WIDE:
        return lax.rem(batch + 3 + 2 * half, 4) * 4 + p - 2
    return lax.rem(batch + 2, 4) * 4 + p - WIDE


def slot_of(batch, group):
    away = lax.rem(group // 4 + 4 - batch, 4)
    piece = lax.rem(group, 4)
    near = 4 + 2 * piece + jnp.where(away == 1, 1, 0)
    return jnp.where(away == 0, piece, jnp.where(away == 2, 12 + piece, near))


def kernel(
    samples, weight, bias, upstream,
    st_out, early_out, g_out, act_out, bias_out,
    st_buf, early_buf, g_buf, s_buf, w_buf, bias_buf,
    a_send_w, a_w, b_send_w, b_w, z_w, c_w,
    a_send_t, a_t, b_send_t, b_t, z_t, c_t, joined,
    part, asm, u_buf, u_pair, act_buf,
    load_sem, w_sem, bias_sem, u_sem, y_send, y_recv, us_sem, ur_sem, uz_send, uz_recv,
    a_send, a_recv, b_send, b_recv, z_send, z_recv, c_send, c_recv, st_sem, early_sem, near_sem,
):
    y_lo, z, x, core = (lax.axis_index(name) for name in SENSOR)
    batch = lax.axis_index("batch")
    mine = 2 * x + core
    up, down = lax.rem(batch + 1, 4), lax.rem(batch + 3, 4)
    other = 1 - y_lo

    def class_peer(d):
        k = lax.rem(mine + d, CLASSES)
        return k, {"x": k // 2, "core": lax.rem(k, 2)}

    def z_peer(d):
        return {"z": lax.rem(z + d, DEPTH)}

    place = DEPTH * y_lo + z

    def place_peer(d):
        there = lax.rem(place + d, 2 * DEPTH)
        return {"y_lo": there // DEPTH, "z": lax.rem(there, DEPTH)}

    class_peers = [class_peer(d)[1] for d in range(1, CLASSES)]
    z_peers = [z_peer(d) for d in range(1, DEPTH)]
    place_peers = [place_peer(d) for d in range(1, 2 * DEPTH)]

    loads = [
        pltpu.make_async_copy(samples.at[pl.ds(PIECE * i, PIECE)], s_buf.at[i], load_sem.at[i]) for i in range(8)
    ]
    load_u = pltpu.make_async_copy(upstream, u_buf.at[z, y_lo], u_sem)
    load_w = pltpu.make_async_copy(weight, w_buf, w_sem)
    load_bias = pltpu.make_async_copy(bias, bias_buf, bias_sem)
    load_u.start()
    for copy in loads:
        copy.start()
    load_bias.start()
    load_w.start()

    barrier = pltpu.get_barrier_semaphore()
    near = [
        {"core": 1 - core},
        {"x": lax.rem(x + 1, 4)},
        {"x": lax.rem(x + 3, 4)},
        {"z": lax.rem(z + 1, DEPTH)},
        {"z": lax.rem(z + DEPTH - 1, DEPTH)},
        {"y_lo": other},
    ]
    for device in [{"batch": up}, {"batch": down}, *near]:
        pl.semaphore_signal(barrier, inc=1, device_id=device)

    def hear_further(r):
        for device in near:
            pl.semaphore_signal(near_sem.at[r], inc=1, device_id=device)
        pl.semaphore_wait(near_sem.at[r], len(near))
    load_u.wait()
    for copy in loads:
        copy.wait()
    pl.semaphore_wait(barrier, 2 + len(near))

    u_cross = pltpu.make_async_remote_copy(
        src_ref=u_buf.at[z, y_lo], dst_ref=u_buf.at[z, y_lo], send_sem=us_sem, recv_sem=ur_sem,
        device_id={"y_lo": other},
    )
    u_cross.start()

    def landing(i, direction):
        return 8 + 4 * (i // 2) + 2 * direction + i % 2 if i < 8 else 24 + 2 * (i - 8) + direction

    def y_copy(i, direction):
        source = i if i < 8 else landing(2 * (i - 8) + direction, direction)
        target = landing(i, direction)
        return pltpu.make_async_remote_copy(
            src_ref=s_buf.at[source],
            dst_ref=s_buf.at[target],
            send_sem=y_send.at[direction, i],
            recv_sem=y_recv.at[target],
            device_id={"batch": up if direction == 0 else down},
        )

    def y_start(i):
        for direction in range(2):
            y_copy(i, direction).start()

    def y_arrive(i):
        for direction in range(2):
            y_copy(i, direction).wait_recv()
        if i + AHEAD < PIECES:
            y_start(i + AHEAD)

    for i in range(AHEAD):
        y_start(i)
    load_bias.wait()
    load_w.wait()

    def spread(source, target, send_sem, recv_sem, peers):
        for device in peers:
            pltpu.make_async_remote_copy(
                src_ref=source, dst_ref=target, send_sem=send_sem, recv_sem=recv_sem, device_id=device
            ).start()

    def await_bytes(region, sem):
        pltpu.make_async_copy(region, region, sem).wait()

    def of(wide, thin, p):
        return wide.at[p] if p < WIDE else thin.at[p - WIDE]

    def stage_matmul(p):
        first, count = (4 * p, 4) if p < WIDE else (24 + 2 * (p - WIDE), 2)
        rows = s_buf[first : first + count].reshape(count * PIECE, s_buf.shape[-1])
        part[: count * PIECE] = jnp.dot(rows, w_buf[...], preferred_element_type=jnp.float32)
        outgoing = of(a_send_w, a_send_t, p)
        for half in range(halves(p)):
            for k in range(CLASSES):
                outgoing[k, OWNED * half : OWNED * (half + 1), :] = part[
                    ROWS * half + OWNED * k : ROWS * half + OWNED * (k + 1), :
                ]
        for d in range(1, CLASSES):
            k, device = class_peer(d)
            spread(outgoing.at[k], of(a_w, a_t, p).at[mine], a_send.at[p], a_recv.at[p], [device])

    def stage_class_sum(p):
        incoming = of(a_w, a_t, p)
        await_bytes(incoming.at[pl.ds(0, CLASSES - 1)], a_recv.at[p])
        total = of(a_send_w, a_send_t, p)[mine]
        for d in range(1, CLASSES):
            total = total + incoming[lax.rem(mine + d, CLASSES)]
        if p in JOINED:
            shares = joined.at[p - JOINED[0]]
            shares[place] = total.astype(jnp.bfloat16)
            spread(shares.at[place], shares.at[place], z_send.at[p], z_recv.at[p], place_peers)
        else:
            shares = of(z_w, z_t, p)
            shares[z] = total
            spread(shares.at[z], shares.at[z], z_send.at[p], z_recv.at[p], z_peers)

    def sum_shares(shares, p):
        count = shares.shape[0]
        await_bytes(shares.at[pl.ds(0, count - 1)], z_recv.at[p])
        total = shares[0].astype(jnp.float32)
        for i in range(1, count):
            total = total + shares[i].astype(jnp.float32)
        return total

    def stage_z_sum(p):
        outgoing = of(b_send_w, b_send_t, p)
        outgoing[...] = sum_shares(of(z_w, z_t, p), p).astype(jnp.bfloat16)
        spread(outgoing, of(b_w, b_t, p), b_send.at[p], b_recv.at[p], [{"y_lo": other}])

    def stage_gradient(p):
        if p in JOINED:
            total = sum_shares(joined.at[p - JOINED[0]], p)
        else:
            incoming = of(b_w, b_t, p)
            await_bytes(incoming, b_recv.at[p])
            total = of(b_send_w, b_send_t, p)[...].astype(jnp.float32) + incoming[...].astype(jnp.float32)
        act = jnp.tanh(total + bias_buf[...][None, :])
        for half in range(halves(p)):
            group = group_of(batch, p, half)
            rows = slice(OWNED * half, OWNED * (half + 1))
            u_pair[rows, :] = u_buf[lax.rem(group, DEPTH), group // DEPTH].astype(jnp.float32)
            act_buf[2 * p + half if p < WIDE else p + WIDE] = act[rows]
        scale = u_pair[: OWNED * halves(p)]
        grads = of(c_w, c_t, p)
        grads[mine] = (scale * (1.0 - act * act)).astype(jnp.bfloat16)
        spread(grads.at[mine], grads.at[mine], c_send.at[p], c_recv.at[p], class_peers)

    def stage_assemble(p):
        incoming = of(c_w, c_t, p)
        await_bytes(incoming.at[pl.ds(0, CLASSES - 1)], c_recv.at[p])
        for k in range(CLASSES):
            grads = incoming[k].astype(jnp.float32)
            for half in range(halves(p)):
                asm[ROWS * half + OWNED * k : ROWS * half + OWNED * (k + 1), :] = grads[
                    OWNED * half : OWNED * (half + 1)
                ]
        size = ROWS * halves(p)
        first = 2 * ROWS * p if p < WIDE else ROWS * (p + WIDE)
        grads = asm[:size]
        late = 4 * ROWS * 2
        if first < late:
            g_buf[first : first + size] = grads.astype(jnp.bfloat16)
        else:
            g_out[first - late : first - late + size] = grads.astype(jnp.bfloat16)
        bias_out[...] += jnp.sum(grads, axis=0, keepdims=True)

    def st_copy(block):
        return pltpu.make_async_copy(st_buf.at[block], st_out.at[block - 2], st_sem.at[block - 2])

    def turn(block):
        rows = s_buf[8 * block : 8 * block + 8].reshape(4 * ROWS, s_buf.shape[-1])
        st_buf[block] = rows.T
        if block >= 2:
            st_copy(block).start()

    def early_copy(t):
        rows = pl.ds(TILE * t, TILE)
        return pltpu.make_async_copy(early_buf.at[rows], early_out.at[rows], early_sem.at[t])

    def early_gradient():
        for t in range(early_buf.shape[0] // TILE):
            rows = pl.ds(TILE * t, TILE)
            turned = jnp.concatenate([st_buf[block, rows] for block in range(2)], axis=1)
            early_buf[rows] = jnp.dot(turned, g_buf[...], preferred_element_type=jnp.float32).astype(jnp.bfloat16)
            early_copy(t).start()

    bias_out[...] = jnp.zeros_like(bias_out)

    matmul, class_sum, z_sum, gradient, assemble = (
        stage_matmul, stage_class_sum, stage_z_sum, stage_gradient, stage_assemble
    )

    hear_further(0)
    hear_further(1)
    matmul(0)
    hear_further(2)
    matmul(1)
    y_arrive(0)
    hear_further(3)
    u_cross.wait()
    spread(u_buf.at[z], u_buf.at[z], uz_send, uz_recv, z_peers)
    y_arrive(1)
    matmul(2)
    class_sum(0)
    class_sum(1)
    y_arrive(2)
    turn(0)
    y_arrive(3)
    matmul(3)
    class_sum(2)
    y_arrive(4)
    z_sum(0)
    y_arrive(5)
    matmul(4)
    z_sum(1)
    class_sum(3)
    y_arrive(6)
    z_sum(2)
    turn(1)
    await_bytes(u_buf.at[pl.ds(0, DEPTH - 1)], uz_recv)
    y_arrive(7)
    matmul(5)
    class_sum(4)
    gradient(0)
    y_arrive(8)
    matmul(6)
    z_sum(3)
    gradient(1)
    y_arrive(9)
    matmul(7)
    class_sum(5)
    assemble(0)
    gradient(2)
    class_sum(6)
    y_arrive(10)
    matmul(8)
    z_sum(4)
    assemble(1)
    turn(2)
    class_sum(7)
    y_arrive(11)
    matmul(9)
    gradient(3)
    z_sum(5)
    class_sum(8)
    z_sum(6)
    assemble(2)
    gradient(4)
    turn(3)
    class_sum(9)
    z_sum(7)
    gradient(5)
    gradient(6)
    assemble(3)
    gradient(7)
    gradient(8)
    early_gradient()
    assemble(4)
    assemble(5)
    gradient(9)
    assemble(6)
    assemble(7)
    assemble(8)
    assemble(9)

    act_out[...] = act_buf[slot_of(batch, y_lo * DEPTH + z)]

    for direction in range(2):
        for i in range(PIECES):
            y_copy(i, direction).wait_send()
    await_bytes(u_buf.at[pl.ds(0, DEPTH - 1)], uz_send)
    for p in range(STEPS):
        await_bytes(of(a_w, a_t, p).at[pl.ds(0, CLASSES - 1)], a_send.at[p])
        if p in JOINED:
            await_bytes(joined.at[p - JOINED[0], pl.ds(0, 2 * DEPTH - 1)], z_send.at[p])
        else:
            await_bytes(of(z_w, z_t, p).at[pl.ds(0, DEPTH - 1)], z_send.at[p])
            await_bytes(of(b_w, b_t, p), b_send.at[p])
        await_bytes(of(c_w, c_t, p).at[pl.ds(0, CLASSES - 1)], c_send.at[p])
    for block in range(2, 4):
        st_copy(block).wait()
    for t in range(early_buf.shape[0] // TILE):
        early_copy(t).wait()


def weight_kernel(st, early, g, act, bias, grad_out, act_out, bias_out):
    rows = jnp.concatenate([st[block] for block in range(2)], axis=1)
    late = jnp.dot(rows, g[...], preferred_element_type=jnp.float32)
    grad_out[...] = (early[...].astype(jnp.float32) + late).astype(jnp.bfloat16)
    act_out[...] = act[...].astype(jnp.bfloat16)
    bias_out[...] = bias[0]


def exchange_buffers(steps, rows, hidden):
    f32, bf16 = jnp.float32, jnp.bfloat16
    return [
        pltpu.VMEM((steps, CLASSES, rows, hidden), f32),
        pltpu.VMEM((steps, CLASSES, rows, hidden), f32),
        pltpu.VMEM((steps, rows, hidden), bf16),
        pltpu.VMEM((steps, rows, hidden), bf16),
        pltpu.VMEM((steps, DEPTH, rows, hidden), f32),
        pltpu.VMEM((steps, CLASSES, rows, hidden), bf16),
    ]


def body(samples, branch_weight, branch_bias, upstream):
    sensors, hidden = branch_weight.shape
    funcs = 4 * samples.shape[0]
    f32, bf16 = jnp.float32, jnp.bfloat16
    dma = pltpu.SemaphoreType.DMA
    turned, early, grads, act, bias_sum = pl.pallas_call(
        kernel,
        out_shape=(
            jax.ShapeDtypeStruct((2, sensors, funcs // 4), bf16),
            jax.ShapeDtypeStruct((sensors, hidden), bf16),
            jax.ShapeDtypeStruct((funcs // 2, hidden), bf16),
            jax.ShapeDtypeStruct((OWNED, hidden), f32),
            jax.ShapeDtypeStruct((1, hidden), f32),
        ),
        in_specs=[pl.BlockSpec(memory_space=pl.ANY)] * 4,
        out_specs=(*[pl.BlockSpec(memory_space=pl.ANY)] * 2, *[pl.BlockSpec(memory_space=pltpu.VMEM)] * 3),
        scratch_shapes=[
            pltpu.VMEM((4, sensors, funcs // 4), bf16),
            pltpu.VMEM((sensors, hidden), bf16),
            pltpu.VMEM((funcs // 2, hidden), bf16),
            pltpu.VMEM((32, PIECE, sensors), bf16),
            pltpu.VMEM((sensors, hidden), bf16),
            pltpu.VMEM((hidden,), f32),
            *exchange_buffers(WIDE, 2 * OWNED, hidden),
            *exchange_buffers(STEPS - WIDE, OWNED, hidden),
            pltpu.VMEM((len(JOINED), 2 * DEPTH, OWNED, hidden), bf16),
            pltpu.VMEM((2 * ROWS, hidden), f32),
            pltpu.VMEM((2 * ROWS, hidden), f32),
            pltpu.VMEM((DEPTH, 2, OWNED, hidden), bf16),
            pltpu.VMEM((2 * OWNED, hidden), f32),
            pltpu.VMEM((16, OWNED, hidden), f32),
            dma((8,)), dma, dma, dma, dma((2, PIECES)), dma((32,)), dma, dma, dma, dma,
            dma((STEPS,)), dma((STEPS,)), dma((STEPS,)), dma((STEPS,)),
            dma((STEPS,)), dma((STEPS,)), dma((STEPS,)), dma((STEPS,)),
            dma((2,)), dma((sensors // TILE,)),
            pltpu.SemaphoreType.REGULAR((4,)),
        ],
        compiler_params=pltpu.CompilerParams(
            collective_id=0, has_side_effects=True, vmem_limit_bytes=63 * 1024 * 1024
        ),
    )(samples, branch_weight, branch_bias, upstream)
    whole = lambda *shape: pl.BlockSpec(shape, lambda t: (0,) * len(shape))
    weight_grad, activation, bias_grad = pl.pallas_call(
        weight_kernel,
        grid=(sensors // TILE,),
        out_shape=(
            jax.ShapeDtypeStruct((sensors, hidden), bf16),
            jax.ShapeDtypeStruct((OWNED, hidden), bf16),
            jax.ShapeDtypeStruct((hidden,), f32),
        ),
        in_specs=[
            pl.BlockSpec((2, TILE, funcs // 4), lambda t: (0, t, 0)),
            pl.BlockSpec((TILE, hidden), lambda t: (t, 0)),
            whole(funcs // 2, hidden),
            whole(OWNED, hidden), whole(1, hidden)],
        out_specs=(pl.BlockSpec((TILE, hidden), lambda t: (t, 0)), whole(OWNED, hidden), whole(hidden)),
    )(turned, early, grads, act, bias_sum)
    return activation, weight_grad, bias_grad


def solution(mesh):
    torus = Mesh(
        mesh.devices.reshape(2, 8, 4, 2, mesh.shape["batch"]),
        (*SENSOR, "batch"),
    )
    in_specs = (P("batch", SENSOR), P(SENSOR, "batch"), P("batch"), P(SENSOR, "batch"))
    out_specs = (P(SENSOR, "batch"), P(SENSOR, "batch"), P("batch"))
    return jax.shard_map(body, mesh=torus, in_specs=in_specs, out_specs=out_specs, check_vma=False)
```

```python
import jax
import jax.numpy as jnp
from jax import lax
from jax.experimental import pallas as pl
from jax.experimental.pallas import tpu as pltpu
from jax.sharding import Mesh
from jax.sharding import PartitionSpec as P

SENSOR = ("y_lo", "z", "x", "core")
STEPS = 10
WIDE = 6
ROWS = 32
PIECE = 16
PIECES = 12
AHEAD = 3
OWNED = 4
CLASSES = 8
DEPTH = 8
TILE = 1024
WEIGHT_TILES = 4
JOINED = (8, 9)


def halves(p):
    return 2 if p < WIDE else 1


def group_of(batch, p, half):
    if p < 2:
        return batch * 4 + 2 * p + half
    if p < WIDE:
        return lax.rem(batch + 3 + 2 * half, 4) * 4 + p - 2
    return lax.rem(batch + 2, 4) * 4 + p - WIDE


def slot_of(batch, group):
    away = lax.rem(group // 4 + 4 - batch, 4)
    piece = lax.rem(group, 4)
    near = 4 + 2 * piece + jnp.where(away == 1, 1, 0)
    return jnp.where(away == 0, piece, jnp.where(away == 2, 12 + piece, near))


def kernel(
    samples, weight, bias, upstream,
    st_out, early_out, g_out, act_out, bias_out,
    st_buf, early_buf, g_buf, s_buf, w_buf, bias_buf,
    a_send_w, a_w, b_send_w, b_w, z_w, c_w,
    a_send_t, a_t, b_send_t, b_t, z_t, c_t, joined,
    part, asm, u_buf, u_pair, act_buf,
    load_sem, w_sem, bias_sem, u_sem, y_send, y_recv, us_sem, ur_sem, uz_send, uz_recv,
    a_send, a_recv, b_send, b_recv, z_send, z_recv, c_send, c_recv, st_sem, early_sem, near_sem,
):
    y_lo, z, x, core = (lax.axis_index(name) for name in SENSOR)
    batch = lax.axis_index("batch")
    mine = 2 * x + core
    up, down = lax.rem(batch + 1, 4), lax.rem(batch + 3, 4)
    other = 1 - y_lo

    def class_peer(d):
        k = lax.rem(mine + d, CLASSES)
        return k, {"x": k // 2, "core": lax.rem(k, 2)}

    def z_peer(d):
        return {"z": lax.rem(z + d, DEPTH)}

    place = DEPTH * y_lo + z

    def place_peer(d):
        there = lax.rem(place + d, 2 * DEPTH)
        return {"y_lo": there // DEPTH, "z": lax.rem(there, DEPTH)}

    class_peers = [class_peer(d)[1] for d in range(1, CLASSES)]
    z_peers = [z_peer(d) for d in range(1, DEPTH)]
    place_peers = [place_peer(d) for d in range(1, 2 * DEPTH)]

    loads = [
        pltpu.make_async_copy(samples.at[pl.ds(PIECE * i, PIECE)], s_buf.at[i], load_sem.at[i]) for i in range(8)
    ]
    load_u = pltpu.make_async_copy(upstream, u_buf.at[z, y_lo], u_sem)
    load_w = pltpu.make_async_copy(weight, w_buf, w_sem)
    load_bias = pltpu.make_async_copy(bias, bias_buf, bias_sem)
    load_u.start()
    for copy in loads:
        copy.start()
    load_bias.start()
    load_w.start()

    barrier = pltpu.get_barrier_semaphore()
    near = [
        {"core": 1 - core},
        {"x": lax.rem(x + 1, 4)},
        {"x": lax.rem(x + 3, 4)},
        {"z": lax.rem(z + 1, DEPTH)},
        {"z": lax.rem(z + DEPTH - 1, DEPTH)},
        {"y_lo": other},
    ]
    for device in [{"batch": up}, {"batch": down}, *near]:
        pl.semaphore_signal(barrier, inc=1, device_id=device)

    def hear_further(r):
        for device in near:
            pl.semaphore_signal(near_sem.at[r], inc=1, device_id=device)
        pl.semaphore_wait(near_sem.at[r], len(near))
    load_u.wait()
    for copy in loads[:AHEAD]:
        copy.wait()
    pl.semaphore_wait(barrier, 2 + len(near))

    u_cross = pltpu.make_async_remote_copy(
        src_ref=u_buf.at[z, y_lo], dst_ref=u_buf.at[z, y_lo], send_sem=us_sem, recv_sem=ur_sem,
        device_id={"y_lo": other},
    )
    u_cross.start()

    def landing(i, direction):
        return 8 + 4 * (i // 2) + 2 * direction + i % 2 if i < 8 else 24 + 2 * (i - 8) + direction

    def y_copy(i, direction):
        source = i if i < 8 else landing(2 * (i - 8) + direction, direction)
        target = landing(i, direction)
        return pltpu.make_async_remote_copy(
            src_ref=s_buf.at[source],
            dst_ref=s_buf.at[target],
            send_sem=y_send.at[direction, i],
            recv_sem=y_recv.at[target],
            device_id={"batch": up if direction == 0 else down},
        )

    def y_start(i):
        for direction in range(2):
            y_copy(i, direction).start()

    def y_arrive(i):
        for direction in range(2):
            y_copy(i, direction).wait_recv()
        if i + AHEAD < PIECES:
            y_start(i + AHEAD)

    for i in range(AHEAD):
        y_start(i)
    for copy in loads[AHEAD:]:
        copy.wait()
    load_bias.wait()
    load_w.wait()

    def spread(source, target, send_sem, recv_sem, peers):
        for device in peers:
            pltpu.make_async_remote_copy(
                src_ref=source, dst_ref=target, send_sem=send_sem, recv_sem=recv_sem, device_id=device
            ).start()

    def await_bytes(region, sem):
        pltpu.make_async_copy(region, region, sem).wait()

    def of(wide, thin, p):
        return wide.at[p] if p < WIDE else thin.at[p - WIDE]

    def stage_matmul(p):
        first, count = (4 * p, 4) if p < WIDE else (24 + 2 * (p - WIDE), 2)
        rows = s_buf[first : first + count].reshape(count * PIECE, s_buf.shape[-1])
        part[: count * PIECE] = jnp.dot(rows, w_buf[...], preferred_element_type=jnp.float32)
        outgoing = of(a_send_w, a_send_t, p)
        for half in range(halves(p)):
            for k in range(CLASSES):
                outgoing[k, OWNED * half : OWNED * (half + 1), :] = part[
                    ROWS * half + OWNED * k : ROWS * half + OWNED * (k + 1), :
                ]
        for d in range(1, CLASSES):
            k, device = class_peer(d)
            spread(outgoing.at[k], of(a_w, a_t, p).at[mine], a_send.at[p], a_recv.at[p], [device])

    def stage_class_sum(p):
        incoming = of(a_w, a_t, p)
        await_bytes(incoming.at[pl.ds(0, CLASSES - 1)], a_recv.at[p])
        total = of(a_send_w, a_send_t, p)[mine]
        for d in range(1, CLASSES):
            total = total + incoming[lax.rem(mine + d, CLASSES)]
        if p in JOINED:
            shares = joined.at[p - JOINED[0]]
            shares[place] = total.astype(jnp.bfloat16)
            spread(shares.at[place], shares.at[place], z_send.at[p], z_recv.at[p], place_peers)
        else:
            shares = of(z_w, z_t, p)
            shares[z] = total
            spread(shares.at[z], shares.at[z], z_send.at[p], z_recv.at[p], z_peers)

    def sum_shares(shares, p):
        count = shares.shape[0]
        await_bytes(shares.at[pl.ds(0, count - 1)], z_recv.at[p])
        total = shares[0].astype(jnp.float32)
        for i in range(1, count):
            total = total + shares[i].astype(jnp.float32)
        return total

    def stage_z_sum(p):
        outgoing = of(b_send_w, b_send_t, p)
        outgoing[...] = sum_shares(of(z_w, z_t, p), p).astype(jnp.bfloat16)
        spread(outgoing, of(b_w, b_t, p), b_send.at[p], b_recv.at[p], [{"y_lo": other}])

    def stage_gradient(p):
        if p in JOINED:
            total = sum_shares(joined.at[p - JOINED[0]], p)
        else:
            incoming = of(b_w, b_t, p)
            await_bytes(incoming, b_recv.at[p])
            total = of(b_send_w, b_send_t, p)[...].astype(jnp.float32) + incoming[...].astype(jnp.float32)
        act = jnp.tanh(total + bias_buf[...][None, :])
        for half in range(halves(p)):
            group = group_of(batch, p, half)
            rows = slice(OWNED * half, OWNED * (half + 1))
            u_pair[rows, :] = u_buf[lax.rem(group, DEPTH), group // DEPTH].astype(jnp.float32)
            act_buf[2 * p + half if p < WIDE else p + WIDE] = act[rows]
        scale = u_pair[: OWNED * halves(p)]
        grads = of(c_w, c_t, p)
        grads[mine] = (scale * (1.0 - act * act)).astype(jnp.bfloat16)
        spread(grads.at[mine], grads.at[mine], c_send.at[p], c_recv.at[p], class_peers)

    def stage_assemble(p):
        incoming = of(c_w, c_t, p)
        await_bytes(incoming.at[pl.ds(0, CLASSES - 1)], c_recv.at[p])
        for k in range(CLASSES):
            grads = incoming[k].astype(jnp.float32)
            for half in range(halves(p)):
                asm[ROWS * half + OWNED * k : ROWS * half + OWNED * (k + 1), :] = grads[
                    OWNED * half : OWNED * (half + 1)
                ]
        size = ROWS * halves(p)
        first = 2 * ROWS * p if p < WIDE else ROWS * (p + WIDE)
        grads = asm[:size]
        late = 4 * ROWS * 2
        if first < late:
            g_buf[first : first + size] = grads.astype(jnp.bfloat16)
        else:
            g_out[first - late : first - late + size] = grads.astype(jnp.bfloat16)
        bias_out[...] += jnp.sum(grads, axis=0, keepdims=True)

    def st_copy(block):
        return pltpu.make_async_copy(st_buf.at[block], st_out.at[block - 2], st_sem.at[block - 2])

    def turn(block):
        rows = s_buf[8 * block : 8 * block + 8].reshape(4 * ROWS, s_buf.shape[-1])
        st_buf[block] = rows.T
        if block >= 2:
            st_copy(block).start()

    def early_copy(t):
        rows = pl.ds(TILE * t, TILE)
        return pltpu.make_async_copy(early_buf.at[rows], early_out.at[rows], early_sem.at[t])

    def early_gradient():
        for t in range(early_buf.shape[0] // TILE):
            rows = pl.ds(TILE * t, TILE)
            turned = jnp.concatenate([st_buf[block, rows] for block in range(2)], axis=1)
            early_buf[rows] = jnp.dot(turned, g_buf[...], preferred_element_type=jnp.float32).astype(jnp.bfloat16)
            early_copy(t).start()

    bias_out[...] = jnp.zeros_like(bias_out)

    matmul, class_sum, z_sum, gradient, assemble = (
        stage_matmul, stage_class_sum, stage_z_sum, stage_gradient, stage_assemble
    )

    hear_further(0)
    hear_further(1)
    matmul(0)
    hear_further(2)
    matmul(1)
    y_arrive(0)
    hear_further(3)
    u_cross.wait()
    spread(u_buf.at[z], u_buf.at[z], uz_send, uz_recv, z_peers)
    y_arrive(1)
    matmul(2)
    class_sum(0)
    class_sum(1)
    y_arrive(2)
    turn(0)
    y_arrive(3)
    matmul(3)
    class_sum(2)
    y_arrive(4)
    z_sum(0)
    y_arrive(5)
    matmul(4)
    z_sum(1)
    class_sum(3)
    y_arrive(6)
    z_sum(2)
    turn(1)
    await_bytes(u_buf.at[pl.ds(0, DEPTH - 1)], uz_recv)
    y_arrive(7)
    matmul(5)
    class_sum(4)
    gradient(0)
    y_arrive(8)
    matmul(6)
    z_sum(3)
    gradient(1)
    y_arrive(9)
    matmul(7)
    class_sum(5)
    assemble(0)
    gradient(2)
    class_sum(6)
    y_arrive(10)
    matmul(8)
    z_sum(4)
    assemble(1)
    turn(2)
    class_sum(7)
    y_arrive(11)
    matmul(9)
    gradient(3)
    z_sum(5)
    class_sum(8)
    z_sum(6)
    assemble(2)
    gradient(4)
    turn(3)
    class_sum(9)
    z_sum(7)
    gradient(5)
    gradient(6)
    assemble(3)
    early_gradient()
    gradient(7)
    gradient(8)
    assemble(4)
    assemble(5)
    gradient(9)
    assemble(6)
    assemble(7)
    assemble(8)
    assemble(9)

    act_out[...] = act_buf[slot_of(batch, y_lo * DEPTH + z)]

    for direction in range(2):
        for i in range(PIECES):
            y_copy(i, direction).wait_send()
    await_bytes(u_buf.at[pl.ds(0, DEPTH - 1)], uz_send)
    for p in range(STEPS):
        await_bytes(of(a_w, a_t, p).at[pl.ds(0, CLASSES - 1)], a_send.at[p])
        if p in JOINED:
            await_bytes(joined.at[p - JOINED[0], pl.ds(0, 2 * DEPTH - 1)], z_send.at[p])
        else:
            await_bytes(of(z_w, z_t, p).at[pl.ds(0, DEPTH - 1)], z_send.at[p])
            await_bytes(of(b_w, b_t, p), b_send.at[p])
        await_bytes(of(c_w, c_t, p).at[pl.ds(0, CLASSES - 1)], c_send.at[p])
    for block in range(2, 4):
        st_copy(block).wait()
    for t in range(early_buf.shape[0] // TILE):
        early_copy(t).wait()


def weight_kernel(
    st, early, g, act, bias, grad_out, act_out, bias_out,
    st_buf, early_buf, g_buf, act_buf, bias_buf, out_buf, load_sem, small_sem, out_sem,
):
    tiles, _, tile, _ = st_buf.shape
    load_g = pltpu.make_async_copy(g, g_buf, small_sem.at[0])
    load_g.start()
    loads = []
    for t in range(tiles):
        rows = pl.ds(tile * t, tile)
        loads.append((
            pltpu.make_async_copy(st.at[:, rows], st_buf.at[t], load_sem.at[0, t]),
            pltpu.make_async_copy(early.at[rows], early_buf.at[t], load_sem.at[1, t]),
        ))
        for copy in loads[t]:
            copy.start()
    small = [
        pltpu.make_async_copy(act, act_buf, small_sem.at[1]),
        pltpu.make_async_copy(bias, bias_buf, small_sem.at[2]),
    ]
    for copy in small:
        copy.start()
    load_g.wait()
    stores = []
    for t in range(tiles):
        for copy in loads[t]:
            copy.wait()
        rows = jnp.concatenate([st_buf[t, block] for block in range(2)], axis=1)
        late = jnp.dot(rows, g_buf[...], preferred_element_type=jnp.float32)
        out_buf[t] = (early_buf[t].astype(jnp.float32) + late).astype(jnp.bfloat16)
        store = pltpu.make_async_copy(out_buf.at[t], grad_out.at[pl.ds(tile * t, tile)], out_sem.at[t])
        store.start()
        stores.append(store)
        if t == 0:
            for copy in small:
                copy.wait()
            act_out[...] = act_buf[...].astype(jnp.bfloat16)
            bias_out[...] = bias_buf[0]
    for store in stores:
        store.wait()


def exchange_buffers(steps, rows, hidden):
    f32, bf16 = jnp.float32, jnp.bfloat16
    return [
        pltpu.VMEM((steps, CLASSES, rows, hidden), f32),
        pltpu.VMEM((steps, CLASSES, rows, hidden), f32),
        pltpu.VMEM((steps, rows, hidden), bf16),
        pltpu.VMEM((steps, rows, hidden), bf16),
        pltpu.VMEM((steps, DEPTH, rows, hidden), f32),
        pltpu.VMEM((steps, CLASSES, rows, hidden), bf16),
    ]


def body(samples, branch_weight, branch_bias, upstream):
    sensors, hidden = branch_weight.shape
    funcs = 4 * samples.shape[0]
    f32, bf16 = jnp.float32, jnp.bfloat16
    dma = pltpu.SemaphoreType.DMA
    turned, early, grads, act, bias_sum = pl.pallas_call(
        kernel,
        out_shape=(
            jax.ShapeDtypeStruct((2, sensors, funcs // 4), bf16),
            jax.ShapeDtypeStruct((sensors, hidden), bf16),
            jax.ShapeDtypeStruct((funcs // 2, hidden), bf16),
            jax.ShapeDtypeStruct((OWNED, hidden), f32),
            jax.ShapeDtypeStruct((1, hidden), f32),
        ),
        in_specs=[pl.BlockSpec(memory_space=pl.ANY)] * 4,
        out_specs=(*[pl.BlockSpec(memory_space=pl.ANY)] * 2, *[pl.BlockSpec(memory_space=pltpu.VMEM)] * 3),
        scratch_shapes=[
            pltpu.VMEM((4, sensors, funcs // 4), bf16),
            pltpu.VMEM((sensors, hidden), bf16),
            pltpu.VMEM((funcs // 2, hidden), bf16),
            pltpu.VMEM((32, PIECE, sensors), bf16),
            pltpu.VMEM((sensors, hidden), bf16),
            pltpu.VMEM((hidden,), f32),
            *exchange_buffers(WIDE, 2 * OWNED, hidden),
            *exchange_buffers(STEPS - WIDE, OWNED, hidden),
            pltpu.VMEM((len(JOINED), 2 * DEPTH, OWNED, hidden), bf16),
            pltpu.VMEM((2 * ROWS, hidden), f32),
            pltpu.VMEM((2 * ROWS, hidden), f32),
            pltpu.VMEM((DEPTH, 2, OWNED, hidden), bf16),
            pltpu.VMEM((2 * OWNED, hidden), f32),
            pltpu.VMEM((16, OWNED, hidden), f32),
            dma((8,)), dma, dma, dma, dma((2, PIECES)), dma((32,)), dma, dma, dma, dma,
            dma((STEPS,)), dma((STEPS,)), dma((STEPS,)), dma((STEPS,)),
            dma((STEPS,)), dma((STEPS,)), dma((STEPS,)), dma((STEPS,)),
            dma((2,)), dma((sensors // TILE,)),
            pltpu.SemaphoreType.REGULAR((4,)),
        ],
        compiler_params=pltpu.CompilerParams(
            collective_id=0, has_side_effects=True, vmem_limit_bytes=63 * 1024 * 1024
        ),
    )(samples, branch_weight, branch_bias, upstream)
    tile = sensors // WEIGHT_TILES
    weight_grad, activation, bias_grad = pl.pallas_call(
        weight_kernel,
        out_shape=(
            jax.ShapeDtypeStruct((sensors, hidden), bf16),
            jax.ShapeDtypeStruct((OWNED, hidden), bf16),
            jax.ShapeDtypeStruct((hidden,), f32),
        ),
        in_specs=[pl.BlockSpec(memory_space=pl.ANY)] * 5,
        out_specs=(pl.BlockSpec(memory_space=pl.ANY), *[pl.BlockSpec(memory_space=pltpu.VMEM)] * 2),
        scratch_shapes=[
            pltpu.VMEM((WEIGHT_TILES, 2, tile, funcs // 4), bf16),
            pltpu.VMEM((WEIGHT_TILES, tile, hidden), bf16),
            pltpu.VMEM((funcs // 2, hidden), bf16),
            pltpu.VMEM((OWNED, hidden), f32),
            pltpu.VMEM((1, hidden), f32),
            pltpu.VMEM((WEIGHT_TILES, tile, hidden), bf16),
            dma((2, WEIGHT_TILES)), dma((3,)), dma((WEIGHT_TILES,)),
        ],
        compiler_params=pltpu.CompilerParams(vmem_limit_bytes=63 * 1024 * 1024),
    )(turned, early, grads, act, bias_sum)
    return activation, weight_grad, bias_grad


def solution(mesh):
    torus = Mesh(
        mesh.devices.reshape(2, 8, 4, 2, mesh.shape["batch"]),
        (*SENSOR, "batch"),
    )
    in_specs = (P("batch", SENSOR), P(SENSOR, "batch"), P("batch"), P(SENSOR, "batch"))
    out_specs = (P(SENSOR, "batch"), P(SENSOR, "batch"), P("batch"))
    return jax.shard_map(body, mesh=torus, in_specs=in_specs, out_specs=out_specs, check_vma=False)
```

```python
import jax
import jax.numpy as jnp
from jax import lax
from jax.experimental import pallas as pl
from jax.experimental.pallas import tpu as pltpu
from jax.sharding import Mesh
from jax.sharding import PartitionSpec as P

SENSOR = ("y_lo", "z", "x", "core")
STEPS = 10
WIDE = 6
ROWS = 32
PIECE = 16
PIECES = 12
AHEAD = 3
OWNED = 4
CLASSES = 8
DEPTH = 8
TILE = 1024
JOINED = (8, 9)


def halves(p):
    return 2 if p < WIDE else 1


def group_of(batch, p, half):
    if p < 2:
        return batch * 4 + 2 * p + half
    if p < WIDE:
        return lax.rem(batch + 3 + 2 * half, 4) * 4 + p - 2
    return lax.rem(batch + 2, 4) * 4 + p - WIDE


def slot_of(batch, group):
    away = lax.rem(group // 4 + 4 - batch, 4)
    piece = lax.rem(group, 4)
    near = 4 + 2 * piece + jnp.where(away == 1, 1, 0)
    return jnp.where(away == 0, piece, jnp.where(away == 2, 12 + piece, near))


def kernel(
    samples, weight, bias, upstream,
    st_out, early_out, g_out, act_out, bias_out,
    st_buf, early_buf, g_buf, s_buf, w_buf, bias_buf,
    a_send_w, a_w, b_send_w, b_w, z_w, c_w,
    a_send_t, a_t, b_send_t, b_t, z_t, c_t, joined,
    part, asm, u_buf, u_pair, act_buf,
    load_sem, w_sem, bias_sem, u_sem, y_send, y_recv, us_sem, ur_sem, uz_send, uz_recv,
    a_send, a_recv, b_send, b_recv, z_send, z_recv, c_send, c_recv, st_sem, early_sem, near_sem,
):
    y_lo, z, x, core = (lax.axis_index(name) for name in SENSOR)
    batch = lax.axis_index("batch")
    mine = 2 * x + core
    up, down = lax.rem(batch + 1, 4), lax.rem(batch + 3, 4)
    other = 1 - y_lo

    def class_peer(d):
        k = lax.rem(mine + d, CLASSES)
        return k, {"x": k // 2, "core": lax.rem(k, 2)}

    def z_peer(d):
        return {"z": lax.rem(z + d, DEPTH)}

    place = DEPTH * y_lo + z

    def place_peer(d):
        there = lax.rem(place + d, 2 * DEPTH)
        return {"y_lo": there // DEPTH, "z": lax.rem(there, DEPTH)}

    class_peers = [class_peer(d)[1] for d in range(1, CLASSES)]
    z_peers = [z_peer(d) for d in range(1, DEPTH)]
    place_peers = [place_peer(d) for d in range(1, 2 * DEPTH)]

    loads = [
        pltpu.make_async_copy(samples.at[pl.ds(PIECE * i, PIECE)], s_buf.at[i], load_sem.at[i]) for i in range(8)
    ]
    load_u = pltpu.make_async_copy(upstream, u_buf.at[z, y_lo], u_sem)
    load_w = pltpu.make_async_copy(weight, w_buf, w_sem)
    load_bias = pltpu.make_async_copy(bias, bias_buf, bias_sem)
    load_u.start()
    for copy in loads:
        copy.start()
    load_bias.start()
    load_w.start()

    barrier = pltpu.get_barrier_semaphore()
    near = [
        {"core": 1 - core},
        {"x": lax.rem(x + 1, 4)},
        {"x": lax.rem(x + 3, 4)},
        {"z": lax.rem(z + 1, DEPTH)},
        {"z": lax.rem(z + DEPTH - 1, DEPTH)},
        {"y_lo": other},
    ]
    for device in [{"batch": up}, {"batch": down}, *near]:
        pl.semaphore_signal(barrier, inc=1, device_id=device)

    def hear_further(r):
        for device in near:
            pl.semaphore_signal(near_sem.at[r], inc=1, device_id=device)
        pl.semaphore_wait(near_sem.at[r], len(near))
    load_u.wait()
    for copy in loads:
        copy.wait()
    pl.semaphore_wait(barrier, 2 + len(near))

    u_cross = pltpu.make_async_remote_copy(
        src_ref=u_buf.at[z, y_lo], dst_ref=u_buf.at[z, y_lo], send_sem=us_sem, recv_sem=ur_sem,
        device_id={"y_lo": other},
    )
    u_cross.start()

    def landing(i, direction):
        return 8 + 4 * (i // 2) + 2 * direction + i % 2 if i < 8 else 24 + 2 * (i - 8) + direction

    def y_copy(i, direction):
        source = i if i < 8 else landing(2 * (i - 8) + direction, direction)
        target = landing(i, direction)
        return pltpu.make_async_remote_copy(
            src_ref=s_buf.at[source],
            dst_ref=s_buf.at[target],
            send_sem=y_send.at[direction, i],
            recv_sem=y_recv.at[target],
            device_id={"batch": up if direction == 0 else down},
        )

    def y_start(i):
        for direction in range(2):
            y_copy(i, direction).start()

    def y_arrive(i):
        for direction in range(2):
            y_copy(i, direction).wait_recv()
        if i + AHEAD < PIECES:
            y_start(i + AHEAD)

    for i in range(AHEAD):
        y_start(i)
    load_bias.wait()
    load_w.wait()

    def spread(source, target, send_sem, recv_sem, peers):
        for device in peers:
            pltpu.make_async_remote_copy(
                src_ref=source, dst_ref=target, send_sem=send_sem, recv_sem=recv_sem, device_id=device
            ).start()

    def await_bytes(region, sem):
        pltpu.make_async_copy(region, region, sem).wait()

    def of(wide, thin, p):
        return wide.at[p] if p < WIDE else thin.at[p - WIDE]

    def stage_matmul(p):
        first, count = (4 * p, 4) if p < WIDE else (24 + 2 * (p - WIDE), 2)
        rows = s_buf[first : first + count].reshape(count * PIECE, s_buf.shape[-1])
        part[: count * PIECE] = jnp.dot(rows, w_buf[...], preferred_element_type=jnp.float32)
        outgoing = of(a_send_w, a_send_t, p)
        for half in range(halves(p)):
            for k in range(CLASSES):
                outgoing[k, OWNED * half : OWNED * (half + 1), :] = part[
                    ROWS * half + OWNED * k : ROWS * half + OWNED * (k + 1), :
                ]
        for d in range(1, CLASSES):
            k, device = class_peer(d)
            spread(outgoing.at[k], of(a_w, a_t, p).at[mine], a_send.at[p], a_recv.at[p], [device])

    def stage_class_sum(p):
        incoming = of(a_w, a_t, p)
        await_bytes(incoming.at[pl.ds(0, CLASSES - 1)], a_recv.at[p])
        total = of(a_send_w, a_send_t, p)[mine]
        for d in range(1, CLASSES):
            total = total + incoming[lax.rem(mine + d, CLASSES)]
        if p in JOINED:
            shares = joined.at[p - JOINED[0]]
            shares[place] = total.astype(jnp.bfloat16)
            spread(shares.at[place], shares.at[place], z_send.at[p], z_recv.at[p], place_peers)
        else:
            shares = of(z_w, z_t, p)
            shares[z] = total
            spread(shares.at[z], shares.at[z], z_send.at[p], z_recv.at[p], z_peers)

    def sum_shares(shares, p):
        count = shares.shape[0]
        await_bytes(shares.at[pl.ds(0, count - 1)], z_recv.at[p])
        total = shares[0].astype(jnp.float32)
        for i in range(1, count):
            total = total + shares[i].astype(jnp.float32)
        return total

    def stage_z_sum(p):
        outgoing = of(b_send_w, b_send_t, p)
        outgoing[...] = sum_shares(of(z_w, z_t, p), p).astype(jnp.bfloat16)
        spread(outgoing, of(b_w, b_t, p), b_send.at[p], b_recv.at[p], [{"y_lo": other}])

    def stage_gradient(p):
        if p in JOINED:
            total = sum_shares(joined.at[p - JOINED[0]], p)
        else:
            incoming = of(b_w, b_t, p)
            await_bytes(incoming, b_recv.at[p])
            total = of(b_send_w, b_send_t, p)[...].astype(jnp.float32) + incoming[...].astype(jnp.float32)
        act = jnp.tanh(total + bias_buf[...][None, :])
        for half in range(halves(p)):
            group = group_of(batch, p, half)
            rows = slice(OWNED * half, OWNED * (half + 1))
            u_pair[rows, :] = u_buf[lax.rem(group, DEPTH), group // DEPTH].astype(jnp.float32)
            act_buf[2 * p + half if p < WIDE else p + WIDE] = act[rows]
        scale = u_pair[: OWNED * halves(p)]
        grads = of(c_w, c_t, p)
        grads[mine] = (scale * (1.0 - act * act)).astype(jnp.bfloat16)
        spread(grads.at[mine], grads.at[mine], c_send.at[p], c_recv.at[p], class_peers)

    def stage_assemble(p):
        incoming = of(c_w, c_t, p)
        await_bytes(incoming.at[pl.ds(0, CLASSES - 1)], c_recv.at[p])
        for k in range(CLASSES):
            grads = incoming[k].astype(jnp.float32)
            for half in range(halves(p)):
                asm[ROWS * half + OWNED * k : ROWS * half + OWNED * (k + 1), :] = grads[
                    OWNED * half : OWNED * (half + 1)
                ]
        size = ROWS * halves(p)
        first = 2 * ROWS * p if p < WIDE else ROWS * (p + WIDE)
        grads = asm[:size]
        late = 4 * ROWS * 2
        if first < late:
            g_buf[first : first + size] = grads.astype(jnp.bfloat16)
        else:
            g_out[first - late : first - late + size] = grads.astype(jnp.bfloat16)
        bias_out[...] += jnp.sum(grads, axis=0, keepdims=True)

    def st_copy(block):
        return pltpu.make_async_copy(st_buf.at[block], st_out.at[block - 2], st_sem.at[block - 2])

    def turn(block):
        rows = s_buf[8 * block : 8 * block + 8].reshape(4 * ROWS, s_buf.shape[-1])
        st_buf[block] = rows.T
        if block >= 2:
            st_copy(block).start()

    def early_copy(t):
        rows = pl.ds(TILE * t, TILE)
        return pltpu.make_async_copy(early_buf.at[rows], early_out.at[rows], early_sem.at[t])

    def early_gradient():
        for t in range(early_buf.shape[0] // TILE):
            rows = pl.ds(TILE * t, TILE)
            turned = jnp.concatenate([st_buf[block, rows] for block in range(2)], axis=1)
            early_buf[rows] = jnp.dot(turned, g_buf[...], preferred_element_type=jnp.float32).astype(jnp.bfloat16)
            early_copy(t).start()

    bias_out[...] = jnp.zeros_like(bias_out)

    matmul, class_sum, z_sum, gradient, assemble = (
        stage_matmul, stage_class_sum, stage_z_sum, stage_gradient, stage_assemble
    )

    hear_further(0)
    hear_further(1)
    matmul(0)
    hear_further(2)
    matmul(1)
    y_arrive(0)
    hear_further(3)
    u_cross.wait()
    spread(u_buf.at[z], u_buf.at[z], uz_send, uz_recv, z_peers)
    y_arrive(1)
    matmul(2)
    class_sum(0)
    class_sum(1)
    y_arrive(2)
    turn(0)
    y_arrive(3)
    matmul(3)
    class_sum(2)
    y_arrive(4)
    z_sum(0)
    y_arrive(5)
    matmul(4)
    z_sum(1)
    class_sum(3)
    y_arrive(6)
    z_sum(2)
    turn(1)
    await_bytes(u_buf.at[pl.ds(0, DEPTH - 1)], uz_recv)
    y_arrive(7)
    matmul(5)
    class_sum(4)
    gradient(0)
    y_arrive(8)
    matmul(6)
    z_sum(3)
    gradient(1)
    y_arrive(9)
    matmul(7)
    class_sum(5)
    assemble(0)
    gradient(2)
    class_sum(6)
    y_arrive(10)
    matmul(8)
    z_sum(4)
    assemble(1)
    turn(2)
    class_sum(7)
    y_arrive(11)
    matmul(9)
    gradient(3)
    z_sum(5)
    class_sum(8)
    z_sum(6)
    assemble(2)
    gradient(4)
    turn(3)
    class_sum(9)
    z_sum(7)
    gradient(5)
    gradient(6)
    assemble(3)
    gradient(7)
    gradient(8)
    assemble(4)
    assemble(5)
    gradient(9)
    early_gradient()
    assemble(6)
    assemble(7)
    assemble(8)
    assemble(9)

    act_out[...] = act_buf[slot_of(batch, y_lo * DEPTH + z)]

    for direction in range(2):
        for i in range(PIECES):
            y_copy(i, direction).wait_send()
    await_bytes(u_buf.at[pl.ds(0, DEPTH - 1)], uz_send)
    for p in range(STEPS):
        await_bytes(of(a_w, a_t, p).at[pl.ds(0, CLASSES - 1)], a_send.at[p])
        if p in JOINED:
            await_bytes(joined.at[p - JOINED[0], pl.ds(0, 2 * DEPTH - 1)], z_send.at[p])
        else:
            await_bytes(of(z_w, z_t, p).at[pl.ds(0, DEPTH - 1)], z_send.at[p])
            await_bytes(of(b_w, b_t, p), b_send.at[p])
        await_bytes(of(c_w, c_t, p).at[pl.ds(0, CLASSES - 1)], c_send.at[p])
    for block in range(2, 4):
        st_copy(block).wait()
    for t in range(early_buf.shape[0] // TILE):
        early_copy(t).wait()


def weight_kernel(st, early, g, act, bias, grad_out, act_out, bias_out):
    rows = jnp.concatenate([st[block] for block in range(2)], axis=1)
    late = jnp.dot(rows, g[...], preferred_element_type=jnp.float32)
    grad_out[...] = (early[...].astype(jnp.float32) + late).astype(jnp.bfloat16)
    act_out[...] = act[...].astype(jnp.bfloat16)
    bias_out[...] = bias[0]


def exchange_buffers(steps, rows, hidden):
    f32, bf16 = jnp.float32, jnp.bfloat16
    return [
        pltpu.VMEM((steps, CLASSES, rows, hidden), f32),
        pltpu.VMEM((steps, CLASSES, rows, hidden), f32),
        pltpu.VMEM((steps, rows, hidden), bf16),
        pltpu.VMEM((steps, rows, hidden), bf16),
        pltpu.VMEM((steps, DEPTH, rows, hidden), f32),
        pltpu.VMEM((steps, CLASSES, rows, hidden), bf16),
    ]


def body(samples, branch_weight, branch_bias, upstream):
    sensors, hidden = branch_weight.shape
    funcs = 4 * samples.shape[0]
    f32, bf16 = jnp.float32, jnp.bfloat16
    dma = pltpu.SemaphoreType.DMA
    turned, early, grads, act, bias_sum = pl.pallas_call(
        kernel,
        out_shape=(
            jax.ShapeDtypeStruct((2, sensors, funcs // 4), bf16),
            jax.ShapeDtypeStruct((sensors, hidden), bf16),
            jax.ShapeDtypeStruct((funcs // 2, hidden), bf16),
            jax.ShapeDtypeStruct((OWNED, hidden), f32),
            jax.ShapeDtypeStruct((1, hidden), f32),
        ),
        in_specs=[pl.BlockSpec(memory_space=pl.ANY)] * 4,
        out_specs=(*[pl.BlockSpec(memory_space=pl.ANY)] * 2, *[pl.BlockSpec(memory_space=pltpu.VMEM)] * 3),
        scratch_shapes=[
            pltpu.VMEM((4, sensors, funcs // 4), bf16),
            pltpu.VMEM((sensors, hidden), bf16),
            pltpu.VMEM((funcs // 2, hidden), bf16),
            pltpu.VMEM((32, PIECE, sensors), bf16),
            pltpu.VMEM((sensors, hidden), bf16),
            pltpu.VMEM((hidden,), f32),
            *exchange_buffers(WIDE, 2 * OWNED, hidden),
            *exchange_buffers(STEPS - WIDE, OWNED, hidden),
            pltpu.VMEM((len(JOINED), 2 * DEPTH, OWNED, hidden), bf16),
            pltpu.VMEM((2 * ROWS, hidden), f32),
            pltpu.VMEM((2 * ROWS, hidden), f32),
            pltpu.VMEM((DEPTH, 2, OWNED, hidden), bf16),
            pltpu.VMEM((2 * OWNED, hidden), f32),
            pltpu.VMEM((16, OWNED, hidden), f32),
            dma((8,)), dma, dma, dma, dma((2, PIECES)), dma((32,)), dma, dma, dma, dma,
            dma((STEPS,)), dma((STEPS,)), dma((STEPS,)), dma((STEPS,)),
            dma((STEPS,)), dma((STEPS,)), dma((STEPS,)), dma((STEPS,)),
            dma((2,)), dma((sensors // TILE,)),
            pltpu.SemaphoreType.REGULAR((4,)),
        ],
        compiler_params=pltpu.CompilerParams(
            collective_id=0, has_side_effects=True, vmem_limit_bytes=63 * 1024 * 1024
        ),
    )(samples, branch_weight, branch_bias, upstream)
    whole = lambda *shape: pl.BlockSpec(shape, lambda t: (0,) * len(shape))
    weight_grad, activation, bias_grad = pl.pallas_call(
        weight_kernel,
        grid=(sensors // TILE,),
        out_shape=(
            jax.ShapeDtypeStruct((sensors, hidden), bf16),
            jax.ShapeDtypeStruct((OWNED, hidden), bf16),
            jax.ShapeDtypeStruct((hidden,), f32),
        ),
        in_specs=[
            pl.BlockSpec((2, TILE, funcs // 4), lambda t: (0, t, 0)),
            pl.BlockSpec((TILE, hidden), lambda t: (t, 0)),
            whole(funcs // 2, hidden),
            whole(OWNED, hidden), whole(1, hidden)],
        out_specs=(pl.BlockSpec((TILE, hidden), lambda t: (t, 0)), whole(OWNED, hidden), whole(hidden)),
    )(turned, early, grads, act, bias_sum)
    return activation, weight_grad, bias_grad


def solution(mesh):
    torus = Mesh(
        mesh.devices.reshape(2, 8, 4, 2, mesh.shape["batch"]),
        (*SENSOR, "batch"),
    )
    in_specs = (P("batch", SENSOR), P(SENSOR, "batch"), P("batch"), P(SENSOR, "batch"))
    out_specs = (P(SENSOR, "batch"), P(SENSOR, "batch"), P("batch"))
    return jax.shard_map(body, mesh=torus, in_specs=in_specs, out_specs=out_specs, check_vma=False)
```

```python
import jax
import jax.numpy as jnp
from jax import lax
from jax.experimental import pallas as pl
from jax.experimental.pallas import tpu as pltpu
from jax.sharding import Mesh
from jax.sharding import PartitionSpec as P

SENSOR = ("y_lo", "z", "x", "core")
STEPS = 10
WIDE = 6
ROWS = 32
PIECE = 16
PIECES = 12
AHEAD = 3
OWNED = 4
CLASSES = 8
DEPTH = 8
TILE = 1024
JOINED = (8, 9)


def halves(p):
    return 2 if p < WIDE else 1


def group_of(batch, p, half):
    if p < 2:
        return batch * 4 + 2 * p + half
    if p < WIDE:
        return lax.rem(batch + 3 + 2 * half, 4) * 4 + p - 2
    return lax.rem(batch + 2, 4) * 4 + p - WIDE


def slot_of(batch, group):
    away = lax.rem(group // 4 + 4 - batch, 4)
    piece = lax.rem(group, 4)
    near = 4 + 2 * piece + jnp.where(away == 1, 1, 0)
    return jnp.where(away == 0, piece, jnp.where(away == 2, 12 + piece, near))


def kernel(
    samples, weight, bias, upstream,
    st_out, early_out, g_out, act_out, bias_out,
    st_buf, early_buf, g_buf, s_buf, w_buf, bias_buf,
    a_send_w, a_w, b_send_w, b_w, z_w, c_w,
    a_send_t, a_t, b_send_t, b_t, z_t, c_t, joined,
    part, asm, u_buf, u_pair, act_buf,
    load_sem, w_sem, bias_sem, u_sem, y_send, y_recv, us_sem, ur_sem, uz_send, uz_recv,
    a_send, a_recv, b_send, b_recv, z_send, z_recv, c_send, c_recv, st_sem, early_sem, near_sem,
):
    y_lo, z, x, core = (lax.axis_index(name) for name in SENSOR)
    batch = lax.axis_index("batch")
    mine = 2 * x + core
    up, down = lax.rem(batch + 1, 4), lax.rem(batch + 3, 4)
    other = 1 - y_lo

    def class_peer(d):
        k = lax.rem(mine + d, CLASSES)
        return k, {"x": k // 2, "core": lax.rem(k, 2)}

    def z_peer(d):
        return {"z": lax.rem(z + d, DEPTH)}

    place = DEPTH * y_lo + z

    def place_peer(d):
        there = lax.rem(place + d, 2 * DEPTH)
        return {"y_lo": there // DEPTH, "z": lax.rem(there, DEPTH)}

    class_peers = [class_peer(d)[1] for d in range(1, CLASSES)]
    z_peers = [z_peer(d) for d in range(1, DEPTH)]
    place_peers = [place_peer(d) for d in range(1, 2 * DEPTH)]

    loads = [
        pltpu.make_async_copy(samples.at[pl.ds(PIECE * i, PIECE)], s_buf.at[i], load_sem.at[i]) for i in range(8)
    ]
    load_u = pltpu.make_async_copy(upstream, u_buf.at[z, y_lo], u_sem)
    load_w = pltpu.make_async_copy(weight, w_buf, w_sem)
    load_bias = pltpu.make_async_copy(bias, bias_buf, bias_sem)
    load_u.start()
    for copy in loads:
        copy.start()
    load_bias.start()
    load_w.start()

    barrier = pltpu.get_barrier_semaphore()
    near = [
        {"core": 1 - core},
        {"x": lax.rem(x + 1, 4)},
        {"x": lax.rem(x + 3, 4)},
        {"z": lax.rem(z + 1, DEPTH)},
        {"z": lax.rem(z + DEPTH - 1, DEPTH)},
        {"y_lo": other},
    ]
    for device in [{"batch": up}, {"batch": down}, *near]:
        pl.semaphore_signal(barrier, inc=1, device_id=device)

    def hear_further(r):
        for device in near:
            pl.semaphore_signal(near_sem.at[r], inc=1, device_id=device)
        pl.semaphore_wait(near_sem.at[r], len(near))
    load_u.wait()
    for copy in loads:
        copy.wait()
    pl.semaphore_wait(barrier, 2 + len(near))

    u_cross = pltpu.make_async_remote_copy(
        src_ref=u_buf.at[z, y_lo], dst_ref=u_buf.at[z, y_lo], send_sem=us_sem, recv_sem=ur_sem,
        device_id={"y_lo": other},
    )
    u_cross.start()

    def landing(i, direction):
        return 8 + 4 * (i // 2) + 2 * direction + i % 2 if i < 8 else 24 + 2 * (i - 8) + direction

    def y_copy(i, direction):
        source = i if i < 8 else landing(2 * (i - 8) + direction, direction)
        target = landing(i, direction)
        return pltpu.make_async_remote_copy(
            src_ref=s_buf.at[source],
            dst_ref=s_buf.at[target],
            send_sem=y_send.at[direction, i],
            recv_sem=y_recv.at[target],
            device_id={"batch": up if direction == 0 else down},
        )

    def y_start(i):
        for direction in range(2):
            y_copy(i, direction).start()

    def y_arrive(i):
        for direction in range(2):
            y_copy(i, direction).wait_recv()
        if i + AHEAD < PIECES:
            y_start(i + AHEAD)

    for i in range(AHEAD):
        y_start(i)
    load_bias.wait()
    load_w.wait()

    def spread(source, target, send_sem, recv_sem, peers):
        for device in peers:
            pltpu.make_async_remote_copy(
                src_ref=source, dst_ref=target, send_sem=send_sem, recv_sem=recv_sem, device_id=device
            ).start()

    def await_bytes(region, sem):
        pltpu.make_async_copy(region, region, sem).wait()

    def of(wide, thin, p):
        return wide.at[p] if p < WIDE else thin.at[p - WIDE]

    def stage_matmul(p):
        first, count = (4 * p, 4) if p < WIDE else (24 + 2 * (p - WIDE), 2)
        rows = s_buf[first : first + count].reshape(count * PIECE, s_buf.shape[-1])
        part[: count * PIECE] = jnp.dot(rows, w_buf[...], preferred_element_type=jnp.float32)
        outgoing = of(a_send_w, a_send_t, p)
        for half in range(halves(p)):
            for k in range(CLASSES):
                outgoing[k, OWNED * half : OWNED * (half + 1), :] = part[
                    ROWS * half + OWNED * k : ROWS * half + OWNED * (k + 1), :
                ]
        for d in range(1, CLASSES):
            k, device = class_peer(d)
            spread(outgoing.at[k], of(a_w, a_t, p).at[mine], a_send.at[p], a_recv.at[p], [device])

    def stage_class_sum(p):
        incoming = of(a_w, a_t, p)
        await_bytes(incoming.at[pl.ds(0, CLASSES - 1)], a_recv.at[p])
        total = of(a_send_w, a_send_t, p)[mine]
        for d in range(1, CLASSES):
            total = total + incoming[lax.rem(mine + d, CLASSES)]
        if p in JOINED:
            shares = joined.at[p - JOINED[0]]
            shares[place] = total.astype(jnp.bfloat16)
            spread(shares.at[place], shares.at[place], z_send.at[p], z_recv.at[p], place_peers)
        else:
            shares = of(z_w, z_t, p)
            shares[z] = total
            spread(shares.at[z], shares.at[z], z_send.at[p], z_recv.at[p], z_peers)

    def sum_shares(shares, p):
        count = shares.shape[0]
        await_bytes(shares.at[pl.ds(0, count - 1)], z_recv.at[p])
        total = shares[0].astype(jnp.float32)
        for i in range(1, count):
            total = total + shares[i].astype(jnp.float32)
        return total

    def stage_z_sum(p):
        outgoing = of(b_send_w, b_send_t, p)
        outgoing[...] = sum_shares(of(z_w, z_t, p), p).astype(jnp.bfloat16)
        spread(outgoing, of(b_w, b_t, p), b_send.at[p], b_recv.at[p], [{"y_lo": other}])

    def stage_gradient(p):
        if p in JOINED:
            total = sum_shares(joined.at[p - JOINED[0]], p)
        else:
            incoming = of(b_w, b_t, p)
            await_bytes(incoming, b_recv.at[p])
            total = of(b_send_w, b_send_t, p)[...].astype(jnp.float32) + incoming[...].astype(jnp.float32)
        act = jnp.tanh(total + bias_buf[...][None, :])
        for half in range(halves(p)):
            group = group_of(batch, p, half)
            rows = slice(OWNED * half, OWNED * (half + 1))
            u_pair[rows, :] = u_buf[lax.rem(group, DEPTH), group // DEPTH].astype(jnp.float32)
            act_buf[2 * p + half if p < WIDE else p + WIDE] = act[rows]
        scale = u_pair[: OWNED * halves(p)]
        grads = of(c_w, c_t, p)
        grads[mine] = (scale * (1.0 - act * act)).astype(jnp.bfloat16)
        spread(grads.at[mine], grads.at[mine], c_send.at[p], c_recv.at[p], class_peers)

    def stage_assemble(p):
        incoming = of(c_w, c_t, p)
        await_bytes(incoming.at[pl.ds(0, CLASSES - 1)], c_recv.at[p])
        for k in range(CLASSES):
            grads = incoming[k].astype(jnp.float32)
            for half in range(halves(p)):
                asm[ROWS * half + OWNED * k : ROWS * half + OWNED * (k + 1), :] = grads[
                    OWNED * half : OWNED * (half + 1)
                ]
        size = ROWS * halves(p)
        first = 2 * ROWS * p if p < WIDE else ROWS * (p + WIDE)
        grads = asm[:size]
        late = 4 * ROWS * 2
        if first < late:
            g_buf[first : first + size] = grads.astype(jnp.bfloat16)
        else:
            g_out[first - late : first - late + size] = grads.astype(jnp.bfloat16)
        bias_out[...] += jnp.sum(grads, axis=0, keepdims=True)

    def st_copy(block):
        return pltpu.make_async_copy(st_buf.at[block], st_out.at[block - 2], st_sem.at[block - 2])

    def turn(block):
        rows = s_buf[8 * block : 8 * block + 8].reshape(4 * ROWS, s_buf.shape[-1])
        st_buf[block] = rows.T
        if block >= 2:
            st_copy(block).start()

    def early_copy(t):
        rows = pl.ds(TILE * t, TILE)
        return pltpu.make_async_copy(early_buf.at[rows], early_out.at[rows], early_sem.at[t])

    def early_gradient():
        for t in range(early_buf.shape[0] // TILE):
            rows = pl.ds(TILE * t, TILE)
            turned = jnp.concatenate([st_buf[block, rows] for block in range(2)], axis=1)
            early_buf[rows] = jnp.dot(turned, g_buf[...], preferred_element_type=jnp.float32).astype(jnp.bfloat16)
            early_copy(t).start()

    bias_out[...] = jnp.zeros_like(bias_out)

    matmul, class_sum, z_sum, gradient, assemble = (
        stage_matmul, stage_class_sum, stage_z_sum, stage_gradient, stage_assemble
    )

    hear_further(0)
    hear_further(1)
    matmul(0)
    hear_further(2)
    matmul(1)
    y_arrive(0)
    hear_further(3)
    u_cross.wait()
    spread(u_buf.at[z], u_buf.at[z], uz_send, uz_recv, z_peers)
    y_arrive(1)
    matmul(2)
    class_sum(0)
    class_sum(1)
    y_arrive(2)
    turn(0)
    y_arrive(3)
    matmul(3)
    class_sum(2)
    y_arrive(4)
    z_sum(0)
    y_arrive(5)
    matmul(4)
    z_sum(1)
    class_sum(3)
    y_arrive(6)
    z_sum(2)
    turn(1)
    await_bytes(u_buf.at[pl.ds(0, DEPTH - 1)], uz_recv)
    y_arrive(7)
    matmul(5)
    class_sum(4)
    gradient(0)
    y_arrive(8)
    matmul(6)
    z_sum(3)
    gradient(1)
    y_arrive(9)
    matmul(7)
    class_sum(5)
    assemble(0)
    gradient(2)
    class_sum(6)
    y_arrive(10)
    matmul(8)
    z_sum(4)
    assemble(1)
    turn(2)
    class_sum(7)
    y_arrive(11)
    matmul(9)
    z_sum(5)
    class_sum(8)
    z_sum(6)
    assemble(2)
    turn(3)
    class_sum(9)
    z_sum(7)
    gradient(3)
    gradient(4)
    gradient(5)
    gradient(6)
    gradient(7)
    gradient(8)
    assemble(3)
    assemble(4)
    gradient(9)
    early_gradient()
    assemble(5)
    assemble(6)
    assemble(7)
    assemble(8)
    assemble(9)

    act_out[...] = act_buf[slot_of(batch, y_lo * DEPTH + z)]

    for direction in range(2):
        for i in range(PIECES):
            y_copy(i, direction).wait_send()
    await_bytes(u_buf.at[pl.ds(0, DEPTH - 1)], uz_send)
    for p in range(STEPS):
        await_bytes(of(a_w, a_t, p).at[pl.ds(0, CLASSES - 1)], a_send.at[p])
        if p in JOINED:
            await_bytes(joined.at[p - JOINED[0], pl.ds(0, 2 * DEPTH - 1)], z_send.at[p])
        else:
            await_bytes(of(z_w, z_t, p).at[pl.ds(0, DEPTH - 1)], z_send.at[p])
            await_bytes(of(b_w, b_t, p), b_send.at[p])
        await_bytes(of(c_w, c_t, p).at[pl.ds(0, CLASSES - 1)], c_send.at[p])
    for block in range(2, 4):
        st_copy(block).wait()
    for t in range(early_buf.shape[0] // TILE):
        early_copy(t).wait()


def weight_kernel(st, early, g, act, bias, grad_out, act_out, bias_out):
    rows = jnp.concatenate([st[block] for block in range(2)], axis=1)
    late = jnp.dot(rows, g[...], preferred_element_type=jnp.float32)
    grad_out[...] = (early[...].astype(jnp.float32) + late).astype(jnp.bfloat16)
    act_out[...] = act[...].astype(jnp.bfloat16)
    bias_out[...] = bias[0]


def exchange_buffers(steps, rows, hidden):
    f32, bf16 = jnp.float32, jnp.bfloat16
    return [
        pltpu.VMEM((steps, CLASSES, rows, hidden), f32),
        pltpu.VMEM((steps, CLASSES, rows, hidden), f32),
        pltpu.VMEM((steps, rows, hidden), bf16),
        pltpu.VMEM((steps, rows, hidden), bf16),
        pltpu.VMEM((steps, DEPTH, rows, hidden), f32),
        pltpu.VMEM((steps, CLASSES, rows, hidden), bf16),
    ]


def body(samples, branch_weight, branch_bias, upstream):
    sensors, hidden = branch_weight.shape
    funcs = 4 * samples.shape[0]
    f32, bf16 = jnp.float32, jnp.bfloat16
    dma = pltpu.SemaphoreType.DMA
    turned, early, grads, act, bias_sum = pl.pallas_call(
        kernel,
        out_shape=(
            jax.ShapeDtypeStruct((2, sensors, funcs // 4), bf16),
            jax.ShapeDtypeStruct((sensors, hidden), bf16),
            jax.ShapeDtypeStruct((funcs // 2, hidden), bf16),
            jax.ShapeDtypeStruct((OWNED, hidden), f32),
            jax.ShapeDtypeStruct((1, hidden), f32),
        ),
        in_specs=[pl.BlockSpec(memory_space=pl.ANY)] * 4,
        out_specs=(*[pl.BlockSpec(memory_space=pl.ANY)] * 2, *[pl.BlockSpec(memory_space=pltpu.VMEM)] * 3),
        scratch_shapes=[
            pltpu.VMEM((4, sensors, funcs // 4), bf16),
            pltpu.VMEM((sensors, hidden), bf16),
            pltpu.VMEM((funcs // 2, hidden), bf16),
            pltpu.VMEM((32, PIECE, sensors), bf16),
            pltpu.VMEM((sensors, hidden), bf16),
            pltpu.VMEM((hidden,), f32),
            *exchange_buffers(WIDE, 2 * OWNED, hidden),
            *exchange_buffers(STEPS - WIDE, OWNED, hidden),
            pltpu.VMEM((len(JOINED), 2 * DEPTH, OWNED, hidden), bf16),
            pltpu.VMEM((2 * ROWS, hidden), f32),
            pltpu.VMEM((2 * ROWS, hidden), f32),
            pltpu.VMEM((DEPTH, 2, OWNED, hidden), bf16),
            pltpu.VMEM((2 * OWNED, hidden), f32),
            pltpu.VMEM((16, OWNED, hidden), f32),
            dma((8,)), dma, dma, dma, dma((2, PIECES)), dma((32,)), dma, dma, dma, dma,
            dma((STEPS,)), dma((STEPS,)), dma((STEPS,)), dma((STEPS,)),
            dma((STEPS,)), dma((STEPS,)), dma((STEPS,)), dma((STEPS,)),
            dma((2,)), dma((sensors // TILE,)),
            pltpu.SemaphoreType.REGULAR((4,)),
        ],
        compiler_params=pltpu.CompilerParams(
            collective_id=0, has_side_effects=True, vmem_limit_bytes=63 * 1024 * 1024
        ),
    )(samples, branch_weight, branch_bias, upstream)
    whole = lambda *shape: pl.BlockSpec(shape, lambda t: (0,) * len(shape))
    weight_grad, activation, bias_grad = pl.pallas_call(
        weight_kernel,
        grid=(sensors // TILE,),
        out_shape=(
            jax.ShapeDtypeStruct((sensors, hidden), bf16),
            jax.ShapeDtypeStruct((OWNED, hidden), bf16),
            jax.ShapeDtypeStruct((hidden,), f32),
        ),
        in_specs=[
            pl.BlockSpec((2, TILE, funcs // 4), lambda t: (0, t, 0)),
            pl.BlockSpec((TILE, hidden), lambda t: (t, 0)),
            whole(funcs // 2, hidden),
            whole(OWNED, hidden), whole(1, hidden)],
        out_specs=(pl.BlockSpec((TILE, hidden), lambda t: (t, 0)), whole(OWNED, hidden), whole(hidden)),
    )(turned, early, grads, act, bias_sum)
    return activation, weight_grad, bias_grad


def solution(mesh):
    torus = Mesh(
        mesh.devices.reshape(2, 8, 4, 2, mesh.shape["batch"]),
        (*SENSOR, "batch"),
    )
    in_specs = (P("batch", SENSOR), P(SENSOR, "batch"), P("batch"), P(SENSOR, "batch"))
    out_specs = (P(SENSOR, "batch"), P(SENSOR, "batch"), P("batch"))
    return jax.shard_map(body, mesh=torus, in_specs=in_specs, out_specs=out_specs, check_vma=False)
```
